1024 devices in a mesh: section: 32 (over y, z_hi), expert: 32 (over z_lo, x, core).
Axes of the slice: x: 4, y: 8, z: 16 (z_hi: 4, z_lo: 4; z = z_hi * 4 + z_lo), core: 2. Of those that a mesh axis runs over, the one named last changes fastest.
Arguments:
- grad_out: bfloat16 [32, 4096, 3584], P('section', 'expert'), may hold values from -6 to 6
- hidden_act: bfloat16 [32, 4096, 1024], P('section', 'expert'), may hold values from -0.29882812 to 0.29882812
- scores: float32 [32, 4096, 32], P('section', 'expert'), may hold values from -8 to 8
- expert_ids: int32 [32, 4096], P('section', 'expert'), may hold values from 0 to 31, as said below
- slot_ids: int32 [32, 4096], P('section', 'expert'), may hold values from 0 to 6, as said below
- counts: int32 [32, 32, 32], P('section'), may hold values from 0 to 7, as said below
- down_weight: bfloat16 [32, 1024, 3584], P('expert'), may hold values from -0.1875 to 0.1875
- router: bfloat16 [32, 3584], replicated, may hold values from -0.8984375 to 0.8984375
Outputs:
- act_grad: bfloat16 [32, 4096, 1024], P('section', 'expert')
- score_grad: float32 [32, 4096, 32], P('section', 'expert')
- upstream_grad: bfloat16 [32, 4096, 3584], P('section', 'expert')
The draws below stay inside these ranges and needn't reach their ends.
Inputs may be any that keep to these rules, and one draw needn't show every extreme that they name: `expert_ids`: the 128 tokens of one device name each expert at most 7 times; in every section one expert gets exactly 7 tokens from every device. `slot_ids`: a token's slot is the number of earlier tokens of its device that name the same expert. counts[s, e] is at most the number of tokens of device s of the section that name expert e, and may be smaller; routes whose slot is not below it are dropped; for the expert that gets 7 tokens from every device it is 7.
All inputs are finite; a program needn't handle non-finite values.
Results may differ from the reference program's by a relative error of at most 0.009.
Values may be sent and summed in bfloat16 or wider, within the bound.
No kernel may reach another device: no remote copies, remote signals or barrier semaphores. Data moves between devices by JAX's collectives and lax.ppermute only.
A program may use at most 32 MiB of HBM per device.

```python
import jax
import jax.numpy as jnp
from jax import lax

D = 3584
FF = 1024
TOK_DEV = 128
TOKENS = 4096
EXPERT_TOTAL = 32
SLOT_LIMIT = 7
N_SECTION = 32
N_EXPERT = 32


def route_table(key):
    base = jax.random.fold_in(key, 7)
    keys = jax.random.split(base, 5)
    block_list = N_SECTION * N_EXPERT
    hottest = jax.random.randint(keys[0], (N_SECTION,), 0, EXPERT_TOTAL)
    level_values = jax.random.randint(keys[1], (N_SECTION, EXPERT_TOTAL), 0, 4)
    expert_range = jnp.arange(EXPERT_TOTAL, dtype=jnp.int32)
    busiest_flag = expert_range[None, :] == hottest[:, None]
    extra_score = level_values * 2048 + jnp.where(busiest_flag, 1 << 20, 0)
    extra_score = jnp.repeat(extra_score, N_EXPERT, axis=0)
    random_jitter = jax.random.randint(keys[2], (block_list, EXPERT_TOTAL, SLOT_LIMIT), 0, 4096)
    sorted_order = (extra_score[:, :, None] + random_jitter).reshape(block_list, EXPERT_TOTAL * SLOT_LIMIT).astype(jnp.int32)
    unused, picked = lax.top_k(sorted_order, TOK_DEV)
    chosen = (picked // SLOT_LIMIT).astype(jnp.int32)
    perm_keys = jax.random.split(keys[3], block_list)
    orders = jax.vmap(lambda one_key: jax.random.permutation(one_key, TOK_DEV))(perm_keys)
    chosen = jnp.take_along_axis(chosen, orders, axis=1)
    same = chosen[:, :, None] == chosen[:, None, :]
    positions = jnp.arange(TOK_DEV, dtype=jnp.int32)
    earlier = positions[None, :] < positions[:, None]
    places = jnp.sum(jnp.where(same & earlier[None, :, :], 1, 0), axis=2).astype(jnp.int32)
    tallies = jnp.sum(jnp.where(chosen[:, :, None] == expert_range[None, None, :], 1, 0), axis=1).astype(jnp.int32)
    tallies = tallies.reshape(N_SECTION, N_EXPERT, EXPERT_TOTAL)
    lowest = max(1, SLOT_LIMIT // 2)
    limits = jax.random.randint(keys[4], (N_SECTION, N_EXPERT, EXPERT_TOTAL), lowest, SLOT_LIMIT + 1).astype(jnp.int32)
    limits = jnp.where(busiest_flag[:, None, :], SLOT_LIMIT, limits).astype(jnp.int32)
    accepted = jnp.minimum(tallies, limits).astype(jnp.int32)
    return (chosen.reshape(N_SECTION, TOKENS), places.reshape(N_SECTION, TOKENS), accepted)


def draw_expert_ids(key, part):
    return route_table(key)[0]


def draw_slot_ids(key, part):
    return route_table(key)[1]


def draw_counts(key, part):
    return route_table(key)[2]


def level_of(own_key, shape, shards, smallest, largest):
    level = 1.0
    for axis_at, parts in shards:
        steps = jax.random.uniform(jax.random.fold_in(jax.random.fold_in(own_key, 6), axis_at), (parts,), jnp.float32, smallest / len(shards), largest / len(shards))
        level = level * jnp.repeat(jnp.exp(steps), shape[axis_at] // parts).reshape((-1,) + (1,) * (len(shape) - 1 - axis_at))
    return level


def normal_values(stream_key, shape, scale, most, pieces=(), held_as=jnp.bfloat16):
    result = scale * jax.random.normal(stream_key, shape, jnp.float32)
    if pieces:
        result = result * level_of(stream_key, shape, pieces, -0.22, 0.18)
    return jnp.clip(result, -most, most).astype(held_as)


def setup_inputs(seed: int = 0) -> dict:
    seeds = jax.random.split(jax.random.key(seed), 9)
    return {
        "grad_out": normal_values(seeds[0], (N_SECTION, TOKENS, D), 1.0, 6.0, ((0, 32), (1, 32))),
        "hidden_act": normal_values(seeds[1], (N_SECTION, TOKENS, FF), 0.05, 0.29882812, ((0, 32), (1, 32))),
        "scores": normal_values(seeds[2], (N_SECTION, TOKENS, EXPERT_TOTAL), 1.5, 8.0, ((0, 32), (1, 32)), jnp.float32),
        "expert_ids": draw_expert_ids(jax.random.fold_in(seeds[8], 71), 0),
        "slot_ids": draw_slot_ids(jax.random.fold_in(seeds[8], 71), 0),
        "counts": draw_counts(jax.random.fold_in(seeds[8], 71), 0),
        "down_weight": normal_values(seeds[6], (EXPERT_TOTAL, FF, D), FF ** -0.5, 0.1875, ((0, 32),)),
        "router": normal_values(seeds[7], (EXPERT_TOTAL, D), 0.15, 0.8984375),
    }


route_scale = 2.5


def one_section(pack, down_weight, router):
    grad_out, hidden_act, scores, expert_ids, slot_ids, counts = pack
    source = (jnp.arange(TOKENS) // TOK_DEV).astype(jnp.int32)
    own_limit = counts[source, expert_ids]
    is_live = slot_ids < own_limit
    onehot = expert_ids[:, None] == jnp.arange(EXPERT_TOTAL, dtype=jnp.int32)[None, :]
    chosen_logit = jnp.sum(jnp.where(onehot, scores, 0.0), axis=1)
    sigmoid_vals = jax.nn.sigmoid(chosen_logit)
    gate_bf = (route_scale * sigmoid_vals).astype(jnp.bfloat16)
    masked = jnp.where(is_live[:, None], grad_out, jnp.zeros_like(grad_out))
    slot_total = N_EXPERT * SLOT_LIMIT
    target = (expert_ids * slot_total + source * SLOT_LIMIT + slot_ids).astype(jnp.int32)
    buffer = jnp.zeros((EXPERT_TOTAL * slot_total, D), jnp.bfloat16).at[target].set(masked, mode="drop")
    buffer = buffer.reshape(EXPERT_TOTAL, slot_total, D)

    def expert_back(pair):
        rows_in, weight = pair
        return jnp.dot(rows_in, weight.T, preferred_element_type=jnp.float32)

    back_rows = lax.map(expert_back, (buffer, down_weight)).reshape(EXPERT_TOTAL * slot_total, FF)
    safe_target = jnp.where(is_live, target, 0).astype(jnp.int32)
    own_back = jnp.where(is_live[:, None], back_rows[safe_target], 0.0)
    act_grad = (gate_bf.astype(jnp.float32)[:, None] * own_back).astype(jnp.bfloat16)
    route_grad = jnp.sum(hidden_act.astype(jnp.float32) * own_back, axis=1)
    slope_term = route_grad * route_scale * sigmoid_vals * (1.0 - sigmoid_vals)
    score_grad = jnp.where(onehot, slope_term[:, None], 0.0)
    score_bf = score_grad.astype(jnp.bfloat16)
    token_grad = (grad_out.astype(jnp.float32) + jnp.dot(score_bf, router, preferred_element_type=jnp.float32)).astype(jnp.bfloat16)
    return act_grad, score_grad, token_grad


def reference(grad_out, hidden_act, scores, expert_ids, slot_ids, counts, down_weight, router):
    def per_section(pack):
        return one_section(pack, down_weight, router)

    act_grad, score_grad, token_grad = lax.map(per_section, (grad_out, hidden_act, scores, expert_ids, slot_ids, counts))
    upstream_grad = jnp.concatenate([token_grad[1:], jnp.zeros_like(token_grad[:1])], axis=0)
    return (act_grad, score_grad, upstream_grad)
```

```python
import jax
import jax.numpy as jnp
from jax import lax
from jax.experimental import pallas as pl
from jax.experimental.pallas import tpu as pltpu
from jax.sharding import Mesh, PartitionSpec as P

route_scale = 2.5
slots = 8
axes = ("y", "zh", "zl", "x", "c")
group = ("x", "c")

NT = (((1,), (1,)), ((), ()))


def prep_kernel(own_ref, chosen_ref, places_ref, counts_ref, tok_ref, near_ref, up_ref, early_ref, late_ref, meta_ref):
    tokens = tok_ref.shape[0]
    half = early_ref.shape[0]
    experts = counts_ref.shape[0]
    rows = near_ref.shape[0]
    own = own_ref[0]
    own_z = own_ref[1]
    chosen = chosen_ref[...]
    places = places_ref[...]
    onehot = lax.broadcasted_iota(jnp.int32, (experts, tokens), 0) == chosen
    own_row = lax.broadcasted_iota(jnp.int32, counts_ref.shape, 0) == own
    own_counts = jnp.where(own_row, counts_ref[...], 0).astype(jnp.float32).astype(jnp.bfloat16)
    picked = jnp.dot(own_counts, onehot.astype(jnp.float32).astype(jnp.bfloat16), preferred_element_type=jnp.float32)
    limit = jnp.sum(picked, axis=0, keepdims=True)
    live = places.astype(jnp.float32) < limit
    offset = (lax.shift_right_logical(chosen, 3) - own_z) & 3
    slot = (chosen & 7) * slots + places
    back_target = jnp.where(live, offset * rows + slot, -1)

    def slot_of(k):
        return jnp.where(live & (offset == k), slot, -1)

    order = lax.broadcasted_iota(jnp.int32, (1, tokens), 1)
    key = (jnp.where(live & (offset == 2), 0, tokens) + order).astype(jnp.float32)
    key_rows = jnp.broadcast_to(key, (tokens, tokens))
    rank = jnp.sum((key_rows.T < key_rows).astype(jnp.float32), axis=0, keepdims=True)
    perm = (lax.broadcasted_iota(jnp.int32, (tokens, tokens), 0) == rank.astype(jnp.int32)).astype(jnp.float32).astype(jnp.bfloat16)
    one_down = slot_of(3).astype(jnp.float32)
    two_down = slot_of(2).astype(jnp.float32)
    row_id = lax.broadcasted_iota(jnp.int32, (8, tokens), 0)
    pair = jnp.where(row_id == 0, one_down, jnp.where(row_id == 1, two_down, 0.0)).astype(jnp.bfloat16)
    moved = lax.dot_general(pair, perm, NT, preferred_element_type=jnp.float32)
    meta = jnp.where(row_id < 2, moved, jnp.where(row_id == 2, rank, back_target.astype(jnp.float32)))
    meta_ref[...] = meta.astype(jnp.int32)

    tok = tok_ref[...]
    slot_id = lax.broadcasted_iota(jnp.int32, (rows, tokens), 0)
    up = (slot_id == slot_of(1)).astype(jnp.float32).astype(jnp.bfloat16)
    up_ref[...] = jnp.dot(up, tok, preferred_element_type=jnp.float32).astype(jnp.bfloat16)
    ordered = jnp.dot(perm, tok, preferred_element_type=jnp.float32).astype(jnp.bfloat16)
    early_ref[...] = ordered[:half]
    late_ref[...] = ordered[half:]
    near = (slot_id == slot_of(0)).astype(jnp.float32).astype(jnp.bfloat16)
    near_ref[...] = jnp.dot(near, tok, preferred_element_type=jnp.float32).astype(jnp.bfloat16)


def pack_both_kernel(meta_ref, early_ref, late_ref, out_ref):
    rows = out_ref.shape[0]
    half = early_ref.shape[0]
    tokens = 2 * half
    pick = lax.broadcasted_iota(jnp.int32, (rows, tokens), 0) == meta_ref[0:1, :]
    pick = pick.astype(jnp.float32).astype(jnp.bfloat16)
    out = jnp.dot(pick[:, :half], early_ref[...], preferred_element_type=jnp.float32)
    out = out + jnp.dot(pick[:, half:], late_ref[...], preferred_element_type=jnp.float32)
    out_ref[...] = out.astype(jnp.bfloat16)


def pack_early_kernel(meta_ref, early_ref, out_ref):
    rows = out_ref.shape[0]
    half = early_ref.shape[0]
    pick = lax.broadcasted_iota(jnp.int32, (rows, half), 0) == meta_ref[1:2, :half]
    pick = pick.astype(jnp.float32).astype(jnp.bfloat16)
    out_ref[...] = jnp.dot(pick, early_ref[...], preferred_element_type=jnp.float32).astype(jnp.bfloat16)


def back_kernel(meta_ref, chosen_ref, scores_ref, hidden_ref, r0_ref, r1_ref, r2_ref, r3_ref, act_ref, score_ref, score_bf_ref):
    tokens = hidden_ref.shape[0]
    experts = scores_ref.shape[0]
    rows = r0_ref.shape[0]
    target = jnp.broadcast_to(meta_ref[3:4, :].astype(jnp.float32), (tokens, tokens)).T[:, :1].astype(jnp.int32)
    own_back = jnp.zeros(hidden_ref.shape, jnp.float32)
    for k, ref in enumerate((r0_ref, r1_ref, r2_ref, r3_ref)):
        lane = lax.broadcasted_iota(jnp.int32, (tokens, rows), 1) + k * rows
        pick = (lane == target).astype(jnp.float32).astype(jnp.bfloat16)
        own_back = own_back + jnp.dot(pick, ref[...], preferred_element_type=jnp.float32)
    onehot = lax.broadcasted_iota(jnp.int32, (experts, tokens), 0) == chosen_ref[...]
    logit = jnp.sum(jnp.where(onehot, scores_ref[...], 0.0), axis=0, keepdims=True)
    sigmoid_vals = jax.nn.sigmoid(logit)
    gate = (route_scale * sigmoid_vals).astype(jnp.bfloat16).astype(jnp.float32)
    gate_col = jnp.broadcast_to(gate, (tokens, tokens)).T[:, :1]
    act_ref[...] = (gate_col * own_back).astype(jnp.bfloat16)
    route = jnp.sum(hidden_ref[...].astype(jnp.float32) * own_back, axis=1, keepdims=True)
    route_row = jnp.broadcast_to(route, (tokens, tokens)).T[:1, :]
    slope = route_row * route_scale * sigmoid_vals * (1.0 - sigmoid_vals)
    score = jnp.where(onehot, slope, 0.0)
    score_ref[...] = score
    score_bf_ref[...] = score.astype(jnp.bfloat16)


def up_kernel(meta_ref, early_ref, late_ref, score_ref, router_ref, out_ref):
    half = early_ref.shape[0]
    tokens = 2 * half
    rank = jnp.broadcast_to(meta_ref[2:3, :].astype(jnp.float32), (tokens, tokens)).T.astype(jnp.int32)
    pick = (lax.broadcasted_iota(jnp.int32, (tokens, tokens), 1) == rank).astype(jnp.float32).astype(jnp.bfloat16)
    scores = score_ref[...].astype(jnp.float32).T.astype(jnp.bfloat16)
    out = jnp.dot(pick[:, :half], early_ref[...], preferred_element_type=jnp.float32)
    out = out + jnp.dot(pick[:, half:], late_ref[...], preferred_element_type=jnp.float32)
    out = out + jnp.dot(scores, router_ref[...], preferred_element_type=jnp.float32)
    out_ref[...] = out.astype(jnp.bfloat16)


def whole(count):
    return [pl.BlockSpec(memory_space=pltpu.VMEM)] * count


def sds(shape, dtype=jnp.bfloat16):
    return jax.ShapeDtypeStruct(shape, dtype)


def on_device(dims, grad_out, hidden_act, scores, expert_ids, slot_ids, counts, down_weight, router):
    ny, nz, nzl, nxc = dims
    tok = grad_out[0]
    tokens, width = tok.shape
    hidden_width = hidden_act.shape[2]
    half = tokens // 2
    rows = nxc * slots
    weight = down_weight[0]
    own = lax.axis_index(("zl", "x", "c"))
    own_ids = jnp.stack([own, lax.axis_index("zl")]).astype(jnp.int32)

    def shift(value, distance, turn, skip=False):
        route = []
        for y in range(ny):
            for z in range(nz):
                if skip and y * nz + z < 4:
                    continue
                to_z = (z + distance) % nz
                to_y = (y + (z + distance) // nz) % ny if turn else y
                for j in range(nxc):
                    route.append(((y * nz + z) * nxc + j, (to_y * nz + to_z) * nxc + j))
        return lax.ppermute(value, axes, route)

    def last_hop(value):
        route = []
        for y in range(ny):
            for z in range(nz):
                at = y * nz + z
                start = (at + 3) % (ny * nz)
                if start < nzl:
                    continue
                to = (at - 1) % (ny * nz)
                for j in range(nxc):
                    route.append((at * nxc + j, to * nxc + j))
        return lax.ppermute(value, axes, route)

    def to_previous(value):
        route = [(s * nxc + j, (s - nzl) * nxc + j) for s in range(nzl, ny * nz) for j in range(nxc)]
        return lax.ppermute(value, axes, route)

    def exchange(value):
        cut = value.reshape(nxc, slots, value.shape[1])
        return lax.all_to_all(cut, group, split_axis=0, concat_axis=0, tiled=True).reshape(value.shape)

    def serve(value):
        return lax.dot_general(value, weight, NT, preferred_element_type=jnp.float32).astype(jnp.bfloat16)

    near, up, early, late, meta = pl.pallas_call(
        prep_kernel,
        out_shape=(sds((rows, width)), sds((rows, width)), sds((half, width)), sds((half, width)), sds((8, tokens), jnp.int32)),
        in_specs=[pl.BlockSpec(memory_space=pltpu.SMEM)] + whole(4),
        out_specs=tuple(whole(5)),
    )(own_ids, expert_ids, slot_ids, counts[0], tok)
    up_got = shift(up, 1, False)
    early1 = shift(early, -1, True)
    late1 = shift(late, -1, True)
    meta1 = shift(meta, -1, True)
    early2 = shift(early1, -1, True)
    late2 = shift(late1, -1, True)
    meta2 = shift(meta1, -1, True)
    meta4 = to_previous(meta)
    early3 = shift(early2, -1, True)
    late3 = shift(late2, -1, True)
    early4 = last_hop(early3)
    late4 = last_hop(late3)
    one = pl.pallas_call(
        pack_both_kernel, out_shape=sds((rows, width)), in_specs=whole(3), out_specs=whole(1)[0]
    )(meta1, early1, late1)
    two = pl.pallas_call(
        pack_early_kernel, out_shape=sds((rows, width)), in_specs=whole(2), out_specs=whole(1)[0]
    )(meta2, early2)
    near_rows = exchange(near)
    up_rows = exchange(up_got)
    one_rows = exchange(one)
    two_rows = exchange(two)
    near_back = serve(near_rows)
    up_back = serve(up_rows)
    one_back = serve(one_rows)
    two_back = serve(two_rows)
    r0 = exchange(near_back)
    r1 = exchange(up_back)
    r3 = exchange(one_back)
    r2 = exchange(two_back)
    r1 = shift(r1, -1, False)
    r3 = shift(r3, 1, True)
    r2 = shift(r2, 2, True)
    act, score, score_bf = pl.pallas_call(
        back_kernel,
        out_shape=(sds((tokens, hidden_width)), sds((scores.shape[2], tokens), jnp.float32), sds((scores.shape[2], tokens))),
        in_specs=whole(8),
        out_specs=tuple(whole(3)),
    )(meta, expert_ids, scores[0].T, hidden_act[0], r0, r1, r2, r3)
    late_score = to_previous(score_bf)
    upstream = pl.pallas_call(
        up_kernel, out_shape=sds((tokens, width)), in_specs=whole(5), out_specs=whole(1)[0]
    )(meta4, early4, late4, late_score, router)
    return act[None], score.T[None], upstream[None]


def solution(mesh):
    cut = Mesh(mesh.devices.reshape(8, 4, 4, 4, 2), axes)
    dims = (8, 16, 4, 8)
    section = ("y", "zh")
    expert = ("zl", "x", "c")
    rows = P(section, expert, None)
    in_specs = (rows, rows, rows, P(section, expert), P(section, expert), P(section, None, None), P(expert, None, None), P())

    def body(*arrays):
        return on_device(dims, *arrays)

    return jax.shard_map(body, mesh=cut, in_specs=in_specs, out_specs=(rows, rows, rows), check_vma=False)
```

```python
import jax
import jax.numpy as jnp
from jax import lax
from jax.experimental import pallas as pl
from jax.experimental.pallas import tpu as pltpu
from jax.sharding import Mesh, PartitionSpec as P


route_scale = 2.5
slots = 8
axes = ("y", "zh", "zl", "x", "c")
group = ("x", "c")
expert_axes = ("zl", "x", "c")

NT = (((1,), (1,)), ((), ()))


def as_pick(mask):
    return mask.astype(jnp.float32).astype(jnp.bfloat16)


def column(row, count):
    return jnp.broadcast_to(row, (count, row.shape[1])).T[:, :1]


def prep_kernel(chosen_ref, places_ref, counts_ref, tok_ref, near_ref, up_ref, early_ref, late_ref, meta_ref):
    tokens, width = tok_ref.shape
    half = late_ref.shape[0]
    experts = counts_ref.shape[0]
    rows = near_ref.shape[0]
    own = lax.axis_index(expert_axes)
    own_z = lax.axis_index("zl")
    chosen = chosen_ref[...]
    places = places_ref[...]
    onehot = lax.broadcasted_iota(jnp.int32, (experts, tokens), 0) == chosen
    own_row = lax.broadcasted_iota(jnp.int32, counts_ref.shape, 0) == own
    own_counts = jnp.where(own_row, counts_ref[...], 0).astype(jnp.float32).astype(jnp.bfloat16)
    picked = jnp.dot(own_counts, as_pick(onehot), preferred_element_type=jnp.float32)
    limit = jnp.sum(picked, axis=0, keepdims=True)
    live = places.astype(jnp.float32) < limit
    offset = (lax.shift_right_logical(chosen, 3) - own_z) & 3
    dest = chosen & 7

    def slot_of(k, pitch, base):
        return jnp.where(live & (offset == k), dest * pitch + base + places, -1)

    order = lax.broadcasted_iota(jnp.int32, (1, tokens), 1)
    key = (jnp.where(live & (offset == 2), 0, tokens) + order).astype(jnp.float32)
    key_rows = jnp.broadcast_to(key, (tokens, tokens))
    rank = jnp.sum((key_rows.T < key_rows).astype(jnp.float32), axis=0, keepdims=True)
    perm = as_pick(lax.broadcasted_iota(jnp.int32, (tokens, tokens), 0) == rank.astype(jnp.int32))
    row_id = lax.broadcasted_iota(jnp.int32, (8, tokens), 0)
    one_down = slot_of(3, 2 * slots, 0).astype(jnp.float32)
    two_down = slot_of(2, 2 * slots, slots).astype(jnp.float32)
    pair = jnp.where(row_id == 0, one_down, jnp.where(row_id == 1, two_down, 0.0)).astype(jnp.bfloat16)
    moved = lax.dot_general(pair, perm, NT, preferred_element_type=jnp.float32)

    tok = tok_ref[...]
    ordered = jnp.dot(perm, tok, preferred_element_type=jnp.float32).astype(jnp.bfloat16)
    early_ref[:half] = ordered[:half]
    early_ref[half:] = jnp.zeros((8, width), jnp.bfloat16)
    table = jnp.where(row_id < 2, moved, jnp.where(row_id == 2, rank, 0.0)).astype(jnp.bfloat16)
    early_ref[half:, :tokens] = table
    late_ref[...] = ordered[half:]
    slot_id = lax.broadcasted_iota(jnp.int32, (rows, tokens), 0)
    up_ref[...] = jnp.dot(as_pick(slot_id == slot_of(1, slots, 0)), tok, preferred_element_type=jnp.float32).astype(jnp.bfloat16)
    near_ref[...] = jnp.dot(as_pick(slot_id == slot_of(0, slots, 0)), tok, preferred_element_type=jnp.float32).astype(jnp.bfloat16)
    back = jnp.where(row_id == 0, slot_of(0, 2 * slots, 0), -1)
    for k in (1, 2, 3):
        back = jnp.where(row_id == k, slot_of(k, slots, 0), back)
    meta_ref[...] = back


def pack_kernel(early1_ref, late1_ref, early2_ref, out_ref):
    rows = out_ref.shape[0]
    half, _ = late1_ref.shape
    tokens = 2 * half
    row = lax.broadcasted_iota(jnp.int32, (rows, tokens), 0)
    one = early1_ref[half:, :tokens].astype(jnp.float32)[0:1, :].astype(jnp.int32)
    two = early2_ref[half:, :tokens].astype(jnp.float32)[1:2, :].astype(jnp.int32)
    pick_one = as_pick(row == one)
    pick_two = as_pick(row == two)
    out = jnp.dot(pick_one[:, :half], early1_ref[:half], preferred_element_type=jnp.float32)
    out = out + jnp.dot(pick_one[:, half:], late1_ref[...], preferred_element_type=jnp.float32)
    out = out + jnp.dot(pick_two[:, :half], early2_ref[:half], preferred_element_type=jnp.float32)
    out_ref[...] = out.astype(jnp.bfloat16)


def back_kernel(meta_ref, chosen_ref, scores_ref, hidden_ref, r0_ref, r1_ref, r2_ref, r3_ref, act_ref, score_ref, score_bf_ref):
    tokens = hidden_ref.shape[0]
    experts = scores_ref.shape[0]
    own_back = jnp.zeros(hidden_ref.shape, jnp.float32)
    for k, ref in enumerate((r0_ref, r1_ref, r2_ref, r3_ref)):
        target = column(meta_ref[k:k + 1, :].astype(jnp.float32), tokens).astype(jnp.int32)
        pick = as_pick(lax.broadcasted_iota(jnp.int32, (tokens, ref.shape[0]), 1) == target)
        own_back = own_back + jnp.dot(pick, ref[...], preferred_element_type=jnp.float32)
    onehot = lax.broadcasted_iota(jnp.int32, (experts, tokens), 0) == chosen_ref[...]
    logit = jnp.sum(jnp.where(onehot, scores_ref[...], 0.0), axis=0, keepdims=True)
    sigmoid_vals = jax.nn.sigmoid(logit)
    gate = (route_scale * sigmoid_vals).astype(jnp.bfloat16).astype(jnp.float32)
    act_ref[...] = (column(gate, tokens) * own_back).astype(jnp.bfloat16)
    route = jnp.sum(hidden_ref[...].astype(jnp.float32) * own_back, axis=1, keepdims=True)
    route_row = jnp.broadcast_to(route, (tokens, tokens)).T[:1, :]
    slope = route_row * route_scale * sigmoid_vals * (1.0 - sigmoid_vals)
    score = jnp.where(onehot, slope, 0.0)
    score_ref[...] = score
    score_bf_ref[...] = score.astype(jnp.bfloat16)


def up_kernel(early_ref, late_ref, score_ref, router_ref, out_ref):
    half = late_ref.shape[0]
    tokens = 2 * half
    rank = column(early_ref[half:, :tokens].astype(jnp.float32)[2:3, :], tokens).astype(jnp.int32)
    pick = as_pick(lax.broadcasted_iota(jnp.int32, (tokens, tokens), 1) == rank)
    scores = score_ref[...].astype(jnp.float32).T.astype(jnp.bfloat16)
    out = jnp.dot(pick[:, :half], early_ref[:half], preferred_element_type=jnp.float32)
    out = out + jnp.dot(pick[:, half:], late_ref[...], preferred_element_type=jnp.float32)
    out = out + jnp.dot(scores, router_ref[...], preferred_element_type=jnp.float32)
    out_ref[...] = out.astype(jnp.bfloat16)


def whole(count):
    return [pl.BlockSpec(memory_space=pltpu.VMEM)] * count


def sds(shape, dtype=jnp.bfloat16):
    return jax.ShapeDtypeStruct(shape, dtype)


def on_device(dims, grad_out, hidden_act, scores, expert_ids, slot_ids, counts, down_weight, router):
    ny, nz, nzl, nxc = dims
    tok = grad_out[0]
    tokens, width = tok.shape
    hidden_width = hidden_act.shape[2]
    half = tokens // 2
    rows = nxc * slots
    places = ny * nz
    weight = down_weight[0]

    def lanes(pairs):
        return [(a * nxc + j, b * nxc + j) for a, b in pairs for j in range(nxc)]

    def along_z(value, distance):
        pairs = [(y * nz + z, y * nz + (z + distance) % nz) for y in range(ny) for z in range(nz)]
        return lax.ppermute(value, axes, lanes(pairs))

    def along_path(value, distance):
        return lax.ppermute(value, axes, lanes([(a, (a + distance) % places) for a in range(places)]))

    def to_end(value, left):
        pairs = [(a, (a - left) % places) for a in range(places) if (a + nzl - left) % places >= nzl]
        return lax.ppermute(value, axes, lanes(pairs))

    def exchange(value):
        return lax.all_to_all(value, group, split_axis=0, concat_axis=0, tiled=True)

    def serve(value):
        flat = value.reshape(nxc * 2 * slots, width)
        out = lax.dot_general(flat, weight, NT, preferred_element_type=jnp.float32).astype(jnp.bfloat16)
        return out.reshape(nxc, 2 * slots, hidden_width)

    def cut(value, k):
        return value[:, k * slots:(k + 1) * slots].reshape(rows, hidden_width)

    near, up, early, late, meta = pl.pallas_call(
        prep_kernel,
        out_shape=(sds((rows, width)), sds((rows, width)), sds((half + 8, width)), sds((half, width)), sds((8, tokens), jnp.int32)),
        in_specs=whole(4),
        out_specs=tuple(whole(5)),
    )(expert_ids, slot_ids, counts[0], tok)
    early1 = along_path(early, -1)
    up_got = along_z(up, 1)
    late1 = along_path(late, -1)
    early2 = along_path(early1, -1)
    first = jnp.concatenate([near.reshape(nxc, slots, width), up_got.reshape(nxc, slots, width)], axis=1)
    first = exchange(first)
    late4 = to_end(late1, 3)
    second = pl.pallas_call(
        pack_kernel, out_shape=sds((2 * rows, width)), in_specs=whole(3), out_specs=whole(1)[0]
    )(early1, late1, early2)
    second = exchange(second.reshape(nxc, 2 * slots, width))
    early4 = to_end(early2, 2)
    first_back = serve(first)
    first_got = exchange(first_back)
    second_back = serve(second)
    second_got = exchange(second_back)
    r1 = cut(first_got, 1)
    r1 = along_z(r1, -1)
    r3 = cut(second_got, 0)
    r2 = cut(second_got, 1)
    r2 = along_path(r2, 2)
    r3 = along_path(r3, 1)
    act, score, score_bf = pl.pallas_call(
        back_kernel,
        out_shape=(sds((tokens, hidden_width)), sds((scores.shape[2], tokens), jnp.float32), sds((scores.shape[2], tokens))),
        in_specs=whole(8),
        out_specs=tuple(whole(3)),
    )(meta, expert_ids, scores[0].T, hidden_act[0], first_got.reshape(2 * rows, hidden_width), r1, r2, r3)
    late_score = to_end(score_bf, nzl)
    upstream = pl.pallas_call(
        up_kernel, out_shape=sds((tokens, width)), in_specs=whole(4), out_specs=whole(1)[0]
    )(early4, late4, late_score, router)
    return act[None], score.T[None], upstream[None]


def solution(mesh):
    cut_mesh = Mesh(mesh.devices.reshape(8, 4, 4, 4, 2), axes)
    dims = (8, 16, 4, 8)
    section = ("y", "zh")
    rows = P(section, expert_axes, None)
    in_specs = (rows, rows, rows, P(section, expert_axes), P(section, expert_axes), P(section, None, None), P(expert_axes, None, None), P())

    def body(*arrays):
        return on_device(dims, *arrays)

    return jax.shard_map(body, mesh=cut_mesh, in_specs=in_specs, out_specs=(rows, rows, rows), check_vma=False)
```

```python
import jax
import jax.numpy as jnp
from jax import lax
from jax.experimental import pallas as pl
from jax.experimental.pallas import tpu as pltpu
from jax.sharding import Mesh, PartitionSpec as P


route_scale = 2.5
slots = 8
axes = ("y", "zh", "zl", "x", "c")
group = ("x", "c")
expert_axes = ("zl", "x", "c")

NT = (((1,), (1,)), ((), ()))


def as_pick(mask):
    return mask.astype(jnp.float32).astype(jnp.bfloat16)


def column(row, count):
    return jnp.broadcast_to(row, (count, row.shape[1])).T[:, :1]


def prep_kernel(chosen_ref, places_ref, counts_ref, tok_ref, first_ref, early_ref, late_ref, meta_ref):
    tokens, width = tok_ref.shape
    half = late_ref.shape[0]
    experts = counts_ref.shape[0]
    rows = first_ref.shape[0]
    own = lax.axis_index(expert_axes)
    own_z = lax.axis_index("zl")
    chosen = chosen_ref[...]
    places = places_ref[...]
    onehot = lax.broadcasted_iota(jnp.int32, (experts, tokens), 0) == chosen
    own_row = lax.broadcasted_iota(jnp.int32, counts_ref.shape, 0) == own
    own_counts = jnp.where(own_row, counts_ref[...], 0).astype(jnp.float32).astype(jnp.bfloat16)
    picked = jnp.dot(own_counts, as_pick(onehot), preferred_element_type=jnp.float32)
    limit = jnp.sum(picked, axis=0, keepdims=True)
    live = places.astype(jnp.float32) < limit
    offset = (lax.shift_right_logical(chosen, 3) - own_z) & 3
    dest = chosen & 7

    def slot_of(k):
        return jnp.where(live & (offset == k), dest * slots + places, -1)

    order = lax.broadcasted_iota(jnp.int32, (1, tokens), 1)
    key = (jnp.where(live & (offset == 2), 0, tokens) + order).astype(jnp.float32)
    key_rows = jnp.broadcast_to(key, (tokens, tokens))
    rank = jnp.sum((key_rows.T < key_rows).astype(jnp.float32), axis=0, keepdims=True)
    perm = as_pick(lax.broadcasted_iota(jnp.int32, (tokens, tokens), 0) == rank.astype(jnp.int32))
    row_id = lax.broadcasted_iota(jnp.int32, (8, tokens), 0)
    one_down = slot_of(3).astype(jnp.float32)
    two_down = slot_of(2).astype(jnp.float32)
    pair = jnp.where(row_id == 0, one_down, jnp.where(row_id == 1, two_down, 0.0)).astype(jnp.bfloat16)
    moved = lax.dot_general(pair, perm, NT, preferred_element_type=jnp.float32)

    tok = tok_ref[...]
    ordered = jnp.dot(perm, tok, preferred_element_type=jnp.float32).astype(jnp.bfloat16)
    early_ref[:half] = ordered[:half]
    early_ref[half:] = jnp.zeros((8, width), jnp.bfloat16)
    table = jnp.where(row_id < 2, moved, jnp.where(row_id == 2, rank, 0.0)).astype(jnp.bfloat16)
    early_ref[half:, :tokens] = table
    late_ref[...] = ordered[half:]
    target = jnp.where(live & (offset < 2), (2 * dest + offset) * slots + places, -1)
    pick = as_pick(lax.broadcasted_iota(jnp.int32, (rows, tokens), 0) == target)
    first_ref[...] = jnp.dot(pick, tok, preferred_element_type=jnp.float32).astype(jnp.bfloat16)
    back = jnp.where(row_id == 0, slot_of(0), -1)
    for k in (1, 2, 3):
        back = jnp.where(row_id == k, slot_of(k), back)
    meta_ref[...] = back


def pack_one_kernel(early_ref, late_ref, out_ref):
    half = late_ref.shape[0]
    tokens = 2 * half
    target = early_ref[half:, :tokens].astype(jnp.float32)[0:1, :].astype(jnp.int32)
    pick = as_pick(lax.broadcasted_iota(jnp.int32, (out_ref.shape[0], tokens), 0) == target)
    out = jnp.dot(pick[:, :half], early_ref[:half], preferred_element_type=jnp.float32)
    out = out + jnp.dot(pick[:, half:], late_ref[...], preferred_element_type=jnp.float32)
    out_ref[...] = out.astype(jnp.bfloat16)


def pack_two_kernel(early_ref, out_ref):
    half = early_ref.shape[0] - 8
    target = early_ref[half:, :2 * half].astype(jnp.float32)[1:2, :].astype(jnp.int32)
    pick = as_pick(lax.broadcasted_iota(jnp.int32, (out_ref.shape[0], 2 * half), 0) == target)
    out_ref[...] = jnp.dot(pick[:, :half], early_ref[:half], preferred_element_type=jnp.float32).astype(jnp.bfloat16)


def serve_kernel(r0_ref, r1_ref, r2_ref, r3_ref, weight_ref, out_ref, held_ref):
    rows = r0_ref.shape[0]
    step = weight_ref.shape[0]

    @pl.when(pl.program_id(0) == 0)
    def _():
        for k, ref in enumerate((r0_ref, r1_ref, r2_ref, r3_ref)):
            held_ref[k * rows:(k + 1) * rows] = ref[...]

    found = lax.dot_general(weight_ref[...], held_ref[...], NT, preferred_element_type=jnp.float32).T
    for k in range(4):
        part = found[k * rows:(k + 1) * rows].reshape(rows // slots, slots, step)
        out_ref[:, k] = part.astype(jnp.bfloat16)


def back_kernel(meta_ref, chosen_ref, scores_ref, hidden_ref, r0_ref, r1_ref, r2_ref, r3_ref, act_ref, score_ref, score_bf_ref):
    tokens = hidden_ref.shape[0]
    experts = scores_ref.shape[0]
    own_back = jnp.zeros(hidden_ref.shape, jnp.float32)
    for k, ref in enumerate((r0_ref, r1_ref, r2_ref, r3_ref)):
        target = column(meta_ref[k:k + 1, :].astype(jnp.float32), tokens).astype(jnp.int32)
        pick = as_pick(lax.broadcasted_iota(jnp.int32, (tokens, ref.shape[0]), 1) == target)
        own_back = own_back + jnp.dot(pick, ref[...], preferred_element_type=jnp.float32)
    onehot = lax.broadcasted_iota(jnp.int32, (experts, tokens), 0) == chosen_ref[...]
    logit = jnp.sum(jnp.where(onehot, scores_ref[...], 0.0), axis=0, keepdims=True)
    sigmoid_vals = jax.nn.sigmoid(logit)
    gate = (route_scale * sigmoid_vals).astype(jnp.bfloat16).astype(jnp.float32)
    act_ref[...] = (column(gate, tokens) * own_back).astype(jnp.bfloat16)
    route = jnp.sum(hidden_ref[...].astype(jnp.float32) * own_back, axis=1, keepdims=True)
    route_row = jnp.broadcast_to(route, (tokens, tokens)).T[:1, :]
    slope = route_row * route_scale * sigmoid_vals * (1.0 - sigmoid_vals)
    score = jnp.where(onehot, slope, 0.0)
    score_ref[...] = score
    score_bf_ref[...] = score.astype(jnp.bfloat16)


def up_kernel(early_ref, late_ref, score_ref, router_ref, out_ref):
    half = late_ref.shape[0]
    tokens = 2 * half
    rank = column(early_ref[half:, :tokens].astype(jnp.float32)[2:3, :], tokens).astype(jnp.int32)
    pick = as_pick(lax.broadcasted_iota(jnp.int32, (tokens, tokens), 1) == rank)
    scores = score_ref[...].astype(jnp.float32).T.astype(jnp.bfloat16)
    out = jnp.dot(pick[:, :half], early_ref[:half], preferred_element_type=jnp.float32)
    out = out + jnp.dot(pick[:, half:], late_ref[...], preferred_element_type=jnp.float32)
    out = out + jnp.dot(scores, router_ref[...], preferred_element_type=jnp.float32)
    out_ref[...] = out.astype(jnp.bfloat16)


def whole(count):
    return [pl.BlockSpec(memory_space=pltpu.VMEM)] * count


def sds(shape, dtype=jnp.bfloat16):
    return jax.ShapeDtypeStruct(shape, dtype)


def on_device(dims, grad_out, hidden_act, scores, expert_ids, slot_ids, counts, down_weight, router):
    ny, nz, nzl, nxc = dims
    tok = grad_out[0]
    tokens, width = tok.shape
    hidden_width = hidden_act.shape[2]
    half = tokens // 2
    rows = nxc * slots
    places = ny * nz
    weight = down_weight[0]

    def lanes(pairs):
        return [(a * nxc + j, b * nxc + j) for a, b in pairs for j in range(nxc)]

    def along_z(value, distance):
        pairs = [(y * nz + z, y * nz + (z + distance) % nz) for y in range(ny) for z in range(nz)]
        return lax.ppermute(value, axes, lanes(pairs))

    def along_path(value, distance):
        return lax.ppermute(value, axes, lanes([(a, (a + distance) % places) for a in range(places)]))

    def to_end(value, left):
        pairs = [(a, (a - left) % places) for a in range(places) if (a + nzl - left) % places >= nzl]
        return lax.ppermute(value, axes, lanes(pairs))

    def exchange(value):
        return lax.all_to_all(value, group, split_axis=0, concat_axis=0, tiled=True)

    def spread(value):
        return exchange(value.reshape(nxc, slots, width)).reshape(rows, width)

    def serve(*values):
        step = hidden_width // 2
        return pl.pallas_call(
            serve_kernel,
            grid=(hidden_width // step,),
            out_shape=sds((nxc, 4, slots, hidden_width)),
            in_specs=[pl.BlockSpec((rows, width), lambda j: (0, 0))] * 4 + [pl.BlockSpec((step, width), lambda j: (j, 0))],
            out_specs=pl.BlockSpec((nxc, 4, slots, step), lambda j: (0, 0, 0, j)),
            scratch_shapes=[pltpu.VMEM((4 * rows, width), jnp.bfloat16)],
        )(*values, weight)

    def part(value, k):
        return value[:, k].reshape(rows, value.shape[3])

    first, early, late, meta = pl.pallas_call(
        prep_kernel,
        out_shape=(sds((2 * rows, width)), sds((half + 8, width)), sds((half, width)), sds((8, tokens), jnp.int32)),
        in_specs=whole(4),
        out_specs=tuple(whole(4)),
    )(expert_ids, slot_ids, counts[0], tok)
    early1 = along_path(early, -1)
    first = exchange(first.reshape(nxc, 2, slots, width))
    late1 = along_path(late, -1)
    early2 = along_path(early1, -1)
    near, up = part(first, 0), part(first, 1)
    up = along_z(up, 1)
    one = pl.pallas_call(
        pack_one_kernel, out_shape=sds((rows, width)), in_specs=whole(2), out_specs=whole(1)[0]
    )(early1, late1)
    one = spread(one)
    late4 = to_end(late1, 3)
    two = pl.pallas_call(
        pack_two_kernel, out_shape=sds((rows, width)), in_specs=whole(1), out_specs=whole(1)[0]
    )(early2)
    two = spread(two)
    early4 = to_end(early2, 2)
    served = serve(near, up, one, two)
    served = exchange(served)
    r0, r1, r3, r2 = (part(served, k) for k in range(4))
    r2 = along_path(r2, 2)
    r1 = along_z(r1, -1)
    r3 = along_path(r3, 1)
    act, score, score_bf = pl.pallas_call(
        back_kernel,
        out_shape=(sds((tokens, hidden_width)), sds((scores.shape[2], tokens), jnp.float32), sds((scores.shape[2], tokens))),
        in_specs=whole(8),
        out_specs=tuple(whole(3)),
    )(meta, expert_ids, scores[0].T, hidden_act[0], r0, r1, r2, r3)
    late_score = to_end(score_bf, nzl)
    upstream = pl.pallas_call(
        up_kernel, out_shape=sds((tokens, width)), in_specs=whole(4), out_specs=whole(1)[0]
    )(early4, late4, late_score, router)
    return act[None], score.T[None], upstream[None]


def solution(mesh):
    cut_mesh = Mesh(mesh.devices.reshape(8, 4, 4, 4, 2), axes)
    dims = (8, 16, 4, 8)
    section = ("y", "zh")
    rows = P(section, expert_axes, None)
    in_specs = (rows, rows, rows, P(section, expert_axes), P(section, expert_axes), P(section, None, None), P(expert_axes, None, None), P())

    def body(*arrays):
        return on_device(dims, *arrays)

    return jax.shard_map(body, mesh=cut_mesh, in_specs=in_specs, out_specs=(rows, rows, rows), check_vma=False)
```

```python
import jax
import jax.numpy as jnp
from jax import lax
from jax.experimental import pallas as pl
from jax.experimental.pallas import tpu as pltpu
from jax.sharding import Mesh, PartitionSpec as P


route_scale = 2.5
slots = 8
axes = ("y", "zh", "zl", "x", "c")
group = ("x", "c")
expert_axes = ("zl", "x", "c")

NT = (((1,), (1,)), ((), ()))


def as_pick(mask):
    return mask.astype(jnp.float32).astype(jnp.bfloat16)


def column(row, count):
    return jnp.broadcast_to(row, (count, row.shape[1])).T[:, :1]


def prep_kernel(chosen_ref, places_ref, counts_ref, tok_ref, first_ref, early_ref, late_ref, meta_ref):
    tokens, width = tok_ref.shape
    half = late_ref.shape[0]
    experts = counts_ref.shape[0]
    rows = first_ref.shape[0]
    own = lax.axis_index(expert_axes)
    own_z = lax.axis_index("zl")
    chosen = chosen_ref[...]
    places = places_ref[...]
    onehot = lax.broadcasted_iota(jnp.int32, (experts, tokens), 0) == chosen
    own_row = lax.broadcasted_iota(jnp.int32, counts_ref.shape, 0) == own
    own_counts = jnp.where(own_row, counts_ref[...], 0).astype(jnp.float32).astype(jnp.bfloat16)
    picked = jnp.dot(own_counts, as_pick(onehot), preferred_element_type=jnp.float32)
    limit = jnp.sum(picked, axis=0, keepdims=True)
    live = places.astype(jnp.float32) < limit
    offset = (lax.shift_right_logical(chosen, 3) - own_z) & 3
    dest = chosen & 7

    def slot_of(k):
        return jnp.where(live & (offset == k), dest * slots + places, -1)

    order = lax.broadcasted_iota(jnp.int32, (1, tokens), 1)
    key = (jnp.where(live & (offset == 2), 0, tokens) + order).astype(jnp.float32)
    key_rows = jnp.broadcast_to(key, (tokens, tokens))
    rank = jnp.sum((key_rows.T < key_rows).astype(jnp.float32), axis=0, keepdims=True)
    perm = as_pick(lax.broadcasted_iota(jnp.int32, (tokens, tokens), 0) == rank.astype(jnp.int32))
    row_id = lax.broadcasted_iota(jnp.int32, (8, tokens), 0)
    one_down = slot_of(3).astype(jnp.float32)
    two_down = slot_of(2).astype(jnp.float32)
    pair = jnp.where(row_id == 0, one_down, jnp.where(row_id == 1, two_down, 0.0)).astype(jnp.bfloat16)
    moved = lax.dot_general(pair, perm, NT, preferred_element_type=jnp.float32)

    tok = tok_ref[...]
    ordered = jnp.dot(perm, tok, preferred_element_type=jnp.float32).astype(jnp.bfloat16)
    early_ref[:half] = ordered[:half]
    early_ref[half:] = jnp.zeros((8, width), jnp.bfloat16)
    table = jnp.where(row_id < 2, moved, jnp.where(row_id == 2, rank, 0.0)).astype(jnp.bfloat16)
    early_ref[half:, :tokens] = table
    late_ref[...] = ordered[half:]
    target = jnp.where(live & (offset < 2), (2 * dest + offset) * slots + places, -1)
    pick = as_pick(lax.broadcasted_iota(jnp.int32, (rows, tokens), 0) == target)
    first_ref[...] = jnp.dot(pick, tok, preferred_element_type=jnp.float32).astype(jnp.bfloat16)
    back = jnp.where(row_id == 0, slot_of(0), -1)
    for k in (1, 2, 3):
        back = jnp.where(row_id == k, slot_of(k), back)
    meta_ref[...] = back


def pack_one_kernel(early_ref, late_ref, out_ref):
    half = late_ref.shape[0]
    tokens = 2 * half
    target = early_ref[half:, :tokens].astype(jnp.float32)[0:1, :].astype(jnp.int32)
    pick = as_pick(lax.broadcasted_iota(jnp.int32, (out_ref.shape[0], tokens), 0) == target)
    out = jnp.dot(pick[:, :half], early_ref[:half], preferred_element_type=jnp.float32)
    out = out + jnp.dot(pick[:, half:], late_ref[...], preferred_element_type=jnp.float32)
    out_ref[...] = out.astype(jnp.bfloat16)


def pack_two_kernel(early_ref, out_ref):
    half = early_ref.shape[0] - 8
    target = early_ref[half:, :2 * half].astype(jnp.float32)[1:2, :].astype(jnp.int32)
    pick = as_pick(lax.broadcasted_iota(jnp.int32, (out_ref.shape[0], 2 * half), 0) == target)
    out_ref[...] = jnp.dot(pick[:, :half], early_ref[:half], preferred_element_type=jnp.float32).astype(jnp.bfloat16)


def serve_kernel(r0_ref, r1_ref, r2_ref, r3_ref, weight_ref, out_ref, held_ref):
    rows = r0_ref.shape[0]
    step = weight_ref.shape[0]

    @pl.when(pl.program_id(0) == 0)
    def _():
        for k, ref in enumerate((r0_ref, r1_ref, r2_ref, r3_ref)):
            held_ref[k * rows:(k + 1) * rows] = ref[...]

    found = lax.dot_general(weight_ref[...], held_ref[...], NT, preferred_element_type=jnp.float32).T
    for k in range(4):
        part = found[k * rows:(k + 1) * rows].reshape(rows // slots, slots, step)
        out_ref[:, k] = part.astype(jnp.bfloat16)


def back_kernel(meta_ref, chosen_ref, scores_ref, hidden_ref, r0_ref, r1_ref, r2_ref, r3_ref, act_ref, score_ref, score_bf_ref):
    tokens = hidden_ref.shape[0]
    experts = scores_ref.shape[0]
    own_back = jnp.zeros(hidden_ref.shape, jnp.float32)
    for k, ref in enumerate((r0_ref, r1_ref, r2_ref, r3_ref)):
        target = column(meta_ref[k:k + 1, :].astype(jnp.float32), tokens).astype(jnp.int32)
        pick = as_pick(lax.broadcasted_iota(jnp.int32, (tokens, ref.shape[0]), 1) == target)
        own_back = own_back + jnp.dot(pick, ref[...], preferred_element_type=jnp.float32)
    onehot = lax.broadcasted_iota(jnp.int32, (experts, tokens), 0) == chosen_ref[...]
    logit = jnp.sum(jnp.where(onehot, scores_ref[...], 0.0), axis=0, keepdims=True)
    sigmoid_vals = jax.nn.sigmoid(logit)
    gate = (route_scale * sigmoid_vals).astype(jnp.bfloat16).astype(jnp.float32)
    act_ref[...] = (column(gate, tokens) * own_back).astype(jnp.bfloat16)
    route = jnp.sum(hidden_ref[...].astype(jnp.float32) * own_back, axis=1, keepdims=True)
    route_row = jnp.broadcast_to(route, (tokens, tokens)).T[:1, :]
    slope = route_row * route_scale * sigmoid_vals * (1.0 - sigmoid_vals)
    score = jnp.where(onehot, slope, 0.0)
    score_ref[...] = score
    score_bf_ref[...] = score.astype(jnp.bfloat16)


def up_kernel(early_ref, late_ref, score_ref, router_ref, out_ref):
    half = late_ref.shape[0]
    tokens = 2 * half
    rank = column(early_ref[half:, :tokens].astype(jnp.float32)[2:3, :], tokens).astype(jnp.int32)
    pick = as_pick(lax.broadcasted_iota(jnp.int32, (tokens, tokens), 1) == rank)
    scores = score_ref[...].astype(jnp.float32).T.astype(jnp.bfloat16)
    out = jnp.dot(pick[:, :half], early_ref[:half], preferred_element_type=jnp.float32)
    out = out + jnp.dot(pick[:, half:], late_ref[...], preferred_element_type=jnp.float32)
    out = out + jnp.dot(scores, router_ref[...], preferred_element_type=jnp.float32)
    out_ref[...] = out.astype(jnp.bfloat16)


def whole(count):
    return [pl.BlockSpec(memory_space=pltpu.VMEM)] * count


def sds(shape, dtype=jnp.bfloat16):
    return jax.ShapeDtypeStruct(shape, dtype)


def on_device(dims, grad_out, hidden_act, scores, expert_ids, slot_ids, counts, down_weight, router):
    ny, nz, nzl, nxc = dims
    tok = grad_out[0]
    tokens, width = tok.shape
    hidden_width = hidden_act.shape[2]
    half = tokens // 2
    rows = nxc * slots
    weight = down_weight[0]

    def lanes(pairs):
        return [(a * nxc + j, b * nxc + j) for a, b in pairs for j in range(nxc)]

    def along_z(value, distance):
        pairs = [(y * nz + z, y * nz + (z + distance) % nz) for y in range(ny) for z in range(nz)]
        return lax.ppermute(value, axes, lanes(pairs))

    def to_end(value, left):
        pairs = []
        for y in range(ny):
            for z in range(nz):
                to = y * nz + (z + nzl - left) % nz - nzl
                if to >= 0:
                    pairs.append((y * nz + z, to))
        return lax.ppermute(value, axes, lanes(pairs))

    def exchange(value):
        return lax.all_to_all(value, group, split_axis=0, concat_axis=0, tiled=True)

    def spread(value):
        return exchange(value.reshape(nxc, slots, width)).reshape(rows, width)

    def serve(*values):
        step = hidden_width // 2
        return pl.pallas_call(
            serve_kernel,
            grid=(hidden_width // step,),
            out_shape=sds((nxc, 4, slots, hidden_width)),
            in_specs=[pl.BlockSpec((rows, width), lambda j: (0, 0))] * 4 + [pl.BlockSpec((step, width), lambda j: (j, 0))],
            out_specs=pl.BlockSpec((nxc, 4, slots, step), lambda j: (0, 0, 0, j)),
            scratch_shapes=[pltpu.VMEM((4 * rows, width), jnp.bfloat16)],
        )(*values, weight)

    def part(value, k):
        return value[:, k].reshape(rows, value.shape[3])

    first, early, late, meta = pl.pallas_call(
        prep_kernel,
        out_shape=(sds((2 * rows, width)), sds((half + 8, width)), sds((half, width)), sds((8, tokens), jnp.int32)),
        in_specs=whole(4),
        out_specs=tuple(whole(4)),
    )(expert_ids, slot_ids, counts[0], tok)
    early1 = along_z(early, -1)
    first = exchange(first.reshape(nxc, 2, slots, width))
    late1 = along_z(late, -1)
    early2 = along_z(early1, -1)
    near, up = part(first, 0), part(first, 1)
    up = along_z(up, 1)
    one = pl.pallas_call(
        pack_one_kernel, out_shape=sds((rows, width)), in_specs=whole(2), out_specs=whole(1)[0]
    )(early1, late1)
    one = spread(one)
    late4 = to_end(late1, 3)
    two = pl.pallas_call(
        pack_two_kernel, out_shape=sds((rows, width)), in_specs=whole(1), out_specs=whole(1)[0]
    )(early2)
    two = spread(two)
    early4 = to_end(early2, 2)
    served = serve(near, up, one, two)
    served = exchange(served)
    r0, r1, r3, r2 = (part(served, k) for k in range(4))
    r2 = along_z(r2, 2)
    r1 = along_z(r1, -1)
    r3 = along_z(r3, 1)
    act, score, score_bf = pl.pallas_call(
        back_kernel,
        out_shape=(sds((tokens, hidden_width)), sds((scores.shape[2], tokens), jnp.float32), sds((scores.shape[2], tokens))),
        in_specs=whole(8),
        out_specs=tuple(whole(3)),
    )(meta, expert_ids, scores[0].T, hidden_act[0], r0, r1, r2, r3)
    late_score = to_end(score_bf, nzl)
    upstream = pl.pallas_call(
        up_kernel, out_shape=sds((tokens, width)), in_specs=whole(4), out_specs=whole(1)[0]
    )(early4, late4, late_score, router)
    return act[None], score.T[None], upstream[None]


def solution(mesh):
    cut_mesh = Mesh(mesh.devices.reshape(8, 4, 4, 4, 2), axes)
    dims = (8, 16, 4, 8)
    section = ("y", "zh")
    rows = P(section, expert_axes, None)
    in_specs = (rows, rows, rows, P(section, expert_axes), P(section, expert_axes), P(section, None, None), P(expert_axes, None, None), P())

    def body(*arrays):
        return on_device(dims, *arrays)

    return jax.shard_map(body, mesh=cut_mesh, in_specs=in_specs, out_specs=(rows, rows, rows), check_vma=False)
```

```python
import jax
import jax.numpy as jnp
from jax import lax
from jax.experimental import pallas as pl
from jax.experimental.pallas import tpu as pltpu
from jax.sharding import Mesh, PartitionSpec as P


route_scale = 2.5
slots = 8
bf16 = jnp.bfloat16
axes = ("y", "zh", "zl", "x", "c")
group = ("x", "c")
expert_axes = ("zl", "x", "c")

NT = (((1,), (1,)), ((), ()))


def as_pick(mask):
    return mask.astype(jnp.float32).astype(jnp.bfloat16)


def column(row, count):
    return jnp.broadcast_to(row, (count, row.shape[1])).T[:, :1]


def prep_kernel(chosen_ref, places_ref, counts_ref, tok_ref, first_ref, early_ref, late_ref, meta_ref):
    tokens, width = tok_ref.shape
    half = late_ref.shape[0]
    experts = counts_ref.shape[0]
    rows = first_ref.shape[0]
    own = lax.axis_index(expert_axes)
    own_z = lax.axis_index("zl")
    chosen = chosen_ref[...]
    places = places_ref[...]
    onehot = lax.broadcasted_iota(jnp.int32, (experts, tokens), 0) == chosen
    own_row = lax.broadcasted_iota(jnp.int32, counts_ref.shape, 0) == own
    own_counts = jnp.where(own_row, counts_ref[...], 0).astype(jnp.float32).astype(jnp.bfloat16)
    picked = jnp.dot(own_counts, as_pick(onehot), preferred_element_type=jnp.float32)
    limit = jnp.sum(picked, axis=0, keepdims=True)
    live = places.astype(jnp.float32) < limit
    offset = (lax.shift_right_logical(chosen, 3) - own_z) & 3
    dest = chosen & 7

    def slot_of(k):
        return jnp.where(live & (offset == k), dest * slots + places, -1)

    order = lax.broadcasted_iota(jnp.int32, (1, tokens), 1)
    key = (jnp.where(live & (offset == 2), 0, tokens) + order).astype(jnp.float32)
    key_rows = jnp.broadcast_to(key, (tokens, tokens))
    rank = jnp.sum((key_rows.T < key_rows).astype(jnp.float32), axis=0, keepdims=True)
    perm = as_pick(lax.broadcasted_iota(jnp.int32, (tokens, tokens), 0) == rank.astype(jnp.int32))
    row_id = lax.broadcasted_iota(jnp.int32, (8, tokens), 0)
    one_down = slot_of(3).astype(jnp.float32)
    two_down = slot_of(2).astype(jnp.float32)
    pair = jnp.where(row_id == 0, one_down, jnp.where(row_id == 1, two_down, 0.0)).astype(jnp.bfloat16)
    moved = lax.dot_general(pair, perm, NT, preferred_element_type=jnp.float32)

    tok = tok_ref[...]
    ordered = jnp.dot(perm, tok, preferred_element_type=jnp.float32).astype(jnp.bfloat16)
    early_ref[:half] = ordered[:half]
    early_ref[half:] = jnp.zeros((8, width), jnp.bfloat16)
    table = jnp.where(row_id < 2, moved, jnp.where(row_id == 2, rank, 0.0)).astype(jnp.bfloat16)
    early_ref[half:, :tokens] = table
    late_ref[...] = ordered[half:]
    target = jnp.where(live & (offset < 2), (2 * dest + offset) * slots + places, -1)
    pick = as_pick(lax.broadcasted_iota(jnp.int32, (rows, tokens), 0) == target)
    first_ref[...] = jnp.dot(pick, tok, preferred_element_type=jnp.float32).astype(jnp.bfloat16)
    back = jnp.where(row_id == 0, slot_of(0), -1)
    for k in (1, 2, 3):
        back = jnp.where(row_id == k, slot_of(k), back)
    meta_ref[...] = back


def pack_one_kernel(early_ref, late_ref, out_ref):
    half = late_ref.shape[0]
    tokens = 2 * half
    target = early_ref[half:, :tokens].astype(jnp.float32)[0:1, :].astype(jnp.int32)
    pick = as_pick(lax.broadcasted_iota(jnp.int32, (out_ref.shape[0], tokens), 0) == target)
    out = jnp.dot(pick[:, :half], early_ref[:half], preferred_element_type=jnp.float32)
    out = out + jnp.dot(pick[:, half:], late_ref[...], preferred_element_type=jnp.float32)
    out_ref[...] = out.astype(jnp.bfloat16)


def pack_two_kernel(early_ref, out_ref):
    half = early_ref.shape[0] - 8
    target = early_ref[half:, :2 * half].astype(jnp.float32)[1:2, :].astype(jnp.int32)
    pick = as_pick(lax.broadcasted_iota(jnp.int32, (out_ref.shape[0], 2 * half), 0) == target)
    out_ref[...] = jnp.dot(pick[:, :half], early_ref[:half], preferred_element_type=jnp.float32).astype(jnp.bfloat16)


def serve_kernel(r0_ref, r1_ref, r2_ref, r3_ref, weight_ref, out_ref, held_ref, fetched_ref, sems):
    rows = r0_ref.shape[0]
    count = sems.shape[0]
    step = weight_ref.shape[0] // count
    blocks = [pl.ds(j * step, step) for j in range(count)]
    fetches = [pltpu.make_async_copy(weight_ref.at[blocks[j]], fetched_ref.at[blocks[j]], sems.at[j]) for j in range(count)]
    for fetch in fetches:
        fetch.start()
    for k, ref in enumerate((r0_ref, r1_ref, r2_ref, r3_ref)):
        held_ref[k * rows:(k + 1) * rows] = ref[...]
    for fetch, block in zip(fetches, blocks):
        fetch.wait()
        found = lax.dot_general(fetched_ref[block, :], held_ref[...], NT, preferred_element_type=jnp.float32).T
        for k in range(4):
            part = found[k * rows:(k + 1) * rows].reshape(rows // slots, slots, step)
            out_ref[:, k, :, block] = part.astype(jnp.bfloat16)


def back_kernel(meta_ref, chosen_ref, scores_ref, hidden_ref, r0_ref, r1_ref, r2_ref, r3_ref, act_ref, score_ref, score_bf_ref):
    tokens = hidden_ref.shape[0]
    experts = scores_ref.shape[0]
    own_back = jnp.zeros(hidden_ref.shape, jnp.float32)
    for k, ref in enumerate((r0_ref, r1_ref, r2_ref, r3_ref)):
        target = column(meta_ref[k:k + 1, :].astype(jnp.float32), tokens).astype(jnp.int32)
        pick = as_pick(lax.broadcasted_iota(jnp.int32, (tokens, ref.shape[0]), 1) == target)
        own_back = own_back + jnp.dot(pick, ref[...], preferred_element_type=jnp.float32)
    onehot = lax.broadcasted_iota(jnp.int32, (experts, tokens), 0) == chosen_ref[...]
    logit = jnp.sum(jnp.where(onehot, scores_ref[...], 0.0), axis=0, keepdims=True)
    sigmoid_vals = jax.nn.sigmoid(logit)
    gate = (route_scale * sigmoid_vals).astype(jnp.bfloat16).astype(jnp.float32)
    act_ref[...] = (column(gate, tokens) * own_back).astype(jnp.bfloat16)
    route = jnp.sum(hidden_ref[...].astype(jnp.float32) * own_back, axis=1, keepdims=True)
    route_row = jnp.broadcast_to(route, (tokens, tokens)).T[:1, :]
    slope = route_row * route_scale * sigmoid_vals * (1.0 - sigmoid_vals)
    score = jnp.where(onehot, slope, 0.0)
    score_ref[...] = score
    score_bf_ref[...] = score.astype(jnp.bfloat16)


def up_kernel(early_ref, late_ref, score_ref, router_ref, out_ref):
    half = late_ref.shape[0]
    tokens = 2 * half
    rank = column(early_ref[half:, :tokens].astype(jnp.float32)[2:3, :], tokens).astype(jnp.int32)
    pick = as_pick(lax.broadcasted_iota(jnp.int32, (tokens, tokens), 1) == rank)
    scores = score_ref[...].astype(jnp.float32).T.astype(jnp.bfloat16)
    out = jnp.dot(pick[:, :half], early_ref[:half], preferred_element_type=jnp.float32)
    out = out + jnp.dot(pick[:, half:], late_ref[...], preferred_element_type=jnp.float32)
    out = out + jnp.dot(scores, router_ref[...], preferred_element_type=jnp.float32)
    out_ref[...] = out.astype(jnp.bfloat16)


def call(kernel, outs, *operands, scratch=()):
    space = {"held": pltpu.VMEM, "near": pltpu.HBM, "far": pltpu.HBM}
    values = [pltpu.with_memory_space_constraint(x, space[how]) for how, x in operands]
    return pl.pallas_call(
        kernel,
        out_shape=tuple(space[how](shape, dtype) for how, shape, dtype in outs),
        in_specs=[pl.BlockSpec(memory_space=pltpu.HBM if how == "far" else pltpu.VMEM) for how, _ in operands],
        out_specs=tuple(pl.BlockSpec(memory_space=pltpu.VMEM) for _ in outs),
        scratch_shapes=scratch,
        compiler_params=pltpu.CompilerParams(vmem_limit_bytes=24 * 1024 * 1024),
    )(*values)


def on_device(dims, grad_out, hidden_act, scores, expert_ids, slot_ids, counts, down_weight, router):
    ny, nz, nzl, nxc = dims
    tok = grad_out[0]
    tokens, width = tok.shape
    hidden_width = hidden_act.shape[2]
    half = tokens // 2
    rows = nxc * slots
    weight = down_weight[0]

    def lanes(pairs):
        return [(a * nxc + j, b * nxc + j) for a, b in pairs for j in range(nxc)]

    def along_z(value, distance):
        pairs = [(y * nz + z, y * nz + (z + distance) % nz) for y in range(ny) for z in range(nz)]
        return lax.ppermute(value, axes, lanes(pairs))

    def to_end(value, left):
        pairs = []
        for y in range(ny):
            for z in range(nz):
                to = y * nz + (z + nzl - left) % nz - nzl
                if to >= 0:
                    pairs.append((y * nz + z, to))
        return lax.ppermute(value, axes, lanes(pairs))

    def exchange(value):
        return lax.all_to_all(value, group, split_axis=0, concat_axis=0, tiled=True)

    def spread(value):
        return exchange(value.reshape(nxc, slots, width)).reshape(rows, width)

    def serve(*values):
        scratch = [
            pltpu.VMEM((4 * rows, width), bf16),
            pltpu.VMEM((hidden_width, width), bf16),
            pltpu.SemaphoreType.DMA((4,)),
        ]
        outs = [("held", (nxc, 4, slots, hidden_width), bf16)]
        return call(serve_kernel, outs, *held(*values), ("far", weight), scratch=scratch)[0]

    def held(*values):
        return [("held", v) for v in values]

    def near_by(*values):
        return [("near", v) for v in values]

    def part(value, k):
        return value[:, k].reshape(rows, value.shape[3])

    outs = [
        ("held", (2 * rows, width), bf16),
        ("held", (half + 8, width), bf16),
        ("held", (half, width), bf16),
        ("near", (8, tokens), jnp.int32),
    ]
    first, early, late, meta = call(prep_kernel, outs, *near_by(expert_ids, slot_ids, counts[0], tok))
    early1 = along_z(early, -1)
    first = exchange(first.reshape(nxc, 2, slots, width))
    late1 = along_z(late, -1)
    early2 = along_z(early1, -1)
    near, up = part(first, 0), part(first, 1)
    up = along_z(up, 1)
    one = call(pack_one_kernel, [("held", (rows, width), bf16)], *held(early1, late1))[0]
    one = spread(one)
    late4 = to_end(late1, 3)
    two = call(pack_two_kernel, [("held", (rows, width), bf16)], *held(early2))[0]
    two = spread(two)
    early4 = to_end(early2, 2)
    served = serve(near, up, one, two)
    served = exchange(served)
    r0, r1, r3, r2 = (part(served, k) for k in range(4))
    r2 = along_z(r2, 2)
    r1 = along_z(r1, -1)
    r3 = along_z(r3, 1)
    experts = scores.shape[2]
    outs = [
        ("near", (tokens, hidden_width), bf16),
        ("near", (experts, tokens), jnp.float32),
        ("held", (experts, tokens), bf16),
    ]
    ins = near_by(meta, expert_ids, scores[0].T, hidden_act[0]) + held(r0, r1, r2, r3)
    act, score, score_bf = call(back_kernel, outs, *ins)
    late_score = to_end(score_bf, nzl)
    upstream = call(up_kernel, [("near", (tokens, width), bf16)], *held(early4, late4, late_score, router))[0]
    return act[None], score.T[None], upstream[None]


def solution(mesh):
    cut_mesh = Mesh(mesh.devices.reshape(8, 4, 4, 4, 2), axes)
    dims = (8, 16, 4, 8)
    section = ("y", "zh")
    rows = P(section, expert_axes, None)
    in_specs = (rows, rows, rows, P(section, expert_axes), P(section, expert_axes), P(section, None, None), P(expert_axes, None, None), P())

    def body(*arrays):
        return on_device(dims, *arrays)

    return jax.shard_map(body, mesh=cut_mesh, in_specs=in_specs, out_specs=(rows, rows, rows), check_vma=False)
```

```python
import jax
import jax.numpy as jnp
from jax import lax
from jax.experimental import pallas as pl
from jax.experimental.pallas import tpu as pltpu
from jax.sharding import Mesh, PartitionSpec as P


route_scale = 2.5
slots = 8
bf16 = jnp.bfloat16
axes = ("y", "zh", "zl", "x", "c")
group = ("x", "c")
expert_axes = ("zl", "x", "c")

NT = (((1,), (1,)), ((), ()))


def as_pick(mask):
    return mask.astype(jnp.float32).astype(jnp.bfloat16)


def column(row, count):
    return jnp.broadcast_to(row, (count, row.shape[1])).T[:, :1]


def prep_kernel(chosen_ref, places_ref, counts_ref, tok_ref, first_ref, early_ref, late_ref, rest_ref, meta_ref):
    tokens, width = tok_ref.shape
    half = early_ref.shape[0] - 8
    last = tokens - rest_ref.shape[0]
    experts = counts_ref.shape[0]
    rows = first_ref.shape[0]
    own = lax.axis_index(expert_axes)
    own_z = lax.axis_index("zl")
    chosen = chosen_ref[...]
    places = places_ref[...]
    onehot = lax.broadcasted_iota(jnp.int32, (experts, tokens), 0) == chosen
    own_row = lax.broadcasted_iota(jnp.int32, counts_ref.shape, 0) == own
    own_counts = jnp.where(own_row, counts_ref[...], 0).astype(jnp.float32).astype(jnp.bfloat16)
    picked = jnp.dot(own_counts, as_pick(onehot), preferred_element_type=jnp.float32)
    limit = jnp.sum(picked, axis=0, keepdims=True)
    live = places.astype(jnp.float32) < limit
    offset = (lax.shift_right_logical(chosen, 3) - own_z) & 3
    dest = chosen & 7

    def slot_of(k):
        return jnp.where(live & (offset == k), dest * slots + places, -1)

    order = lax.broadcasted_iota(jnp.int32, (1, tokens), 1)
    key = (jnp.where(live & (offset >= 2), jnp.where(offset == 2, 0, tokens), 2 * tokens) + order).astype(jnp.float32)
    key_rows = jnp.broadcast_to(key, (tokens, tokens))
    rank = jnp.sum((key_rows.T < key_rows).astype(jnp.float32), axis=0, keepdims=True)
    perm = as_pick(lax.broadcasted_iota(jnp.int32, (tokens, tokens), 0) == rank.astype(jnp.int32))
    row_id = lax.broadcasted_iota(jnp.int32, (8, tokens), 0)
    one_down = slot_of(3).astype(jnp.float32)
    two_down = slot_of(2).astype(jnp.float32)
    pair = jnp.where(row_id == 0, one_down, jnp.where(row_id == 1, two_down, 0.0)).astype(jnp.bfloat16)
    moved = lax.dot_general(pair, perm, NT, preferred_element_type=jnp.float32)

    tok = tok_ref[...]
    ordered = jnp.dot(perm, tok, preferred_element_type=jnp.float32).astype(jnp.bfloat16)
    early_ref[:half] = ordered[:half]
    early_ref[half:] = jnp.zeros((8, width), jnp.bfloat16)
    table = jnp.where(row_id < 2, moved, jnp.where(row_id == 2, rank, 0.0)).astype(jnp.bfloat16)
    early_ref[half:, :tokens] = table
    late_ref[...] = ordered[half:last]
    rest_ref[...] = ordered[last:]
    target = jnp.where(live & (offset < 2), (2 * dest + offset) * slots + places, -1)
    pick = as_pick(lax.broadcasted_iota(jnp.int32, (rows, tokens), 0) == target)
    first_ref[...] = jnp.dot(pick, tok, preferred_element_type=jnp.float32).astype(jnp.bfloat16)
    back = jnp.where(row_id == 0, slot_of(0), -1)
    for k in (1, 2, 3):
        back = jnp.where(row_id == k, slot_of(k), back)
    meta_ref[...] = back


def pack_one_kernel(early_ref, late_ref, out_ref):
    half = early_ref.shape[0] - 8
    count = half + late_ref.shape[0]
    target = early_ref[half:, :2 * half].astype(jnp.float32)[0:1, :].astype(jnp.int32)
    pick = as_pick(lax.broadcasted_iota(jnp.int32, (out_ref.shape[0], 2 * half), 0) == target)
    out = jnp.dot(pick[:, :half], early_ref[:half], preferred_element_type=jnp.float32)
    out = out + jnp.dot(pick[:, half:count], late_ref[...], preferred_element_type=jnp.float32)
    out_ref[...] = out.astype(jnp.bfloat16)


def pack_two_kernel(early_ref, out_ref):
    half = early_ref.shape[0] - 8
    target = early_ref[half:, :2 * half].astype(jnp.float32)[1:2, :].astype(jnp.int32)
    pick = as_pick(lax.broadcasted_iota(jnp.int32, (out_ref.shape[0], 2 * half), 0) == target)
    out_ref[...] = jnp.dot(pick[:, :half], early_ref[:half], preferred_element_type=jnp.float32).astype(jnp.bfloat16)


def serve_part(weight, held, rows):
    found = lax.dot_general(weight, held, NT, preferred_element_type=jnp.float32).T
    parts = []
    for k in range(found.shape[0] // rows):
        part = found[k * rows:(k + 1) * rows].reshape(rows // slots, slots, weight.shape[0])
        parts.append(part.astype(jnp.bfloat16))
    return parts


def fetch_blocks(weight_ref, fetched_ref, sems):
    count = sems.shape[0]
    step = weight_ref.shape[0] // count
    blocks = [pl.ds(j * step, step) for j in range(count)]
    fetches = [pltpu.make_async_copy(weight_ref.at[blocks[j]], fetched_ref.at[blocks[j]], sems.at[j]) for j in range(count)]
    for fetch in fetches:
        fetch.start()
    return list(zip(fetches, blocks))


def serve_three_kernel(r0_ref, r1_ref, r2_ref, weight_ref, out_ref, fetched_ref, held_ref, sems):
    rows = r0_ref.shape[0]
    fetches = fetch_blocks(weight_ref, fetched_ref, sems)
    for k, ref in enumerate((r0_ref, r1_ref, r2_ref)):
        held_ref[k * rows:(k + 1) * rows] = ref[...]
    for fetch, block in fetches:
        fetch.wait()
        for k, part in enumerate(serve_part(fetched_ref[block, :], held_ref[...], rows)):
            out_ref[:, k, :, block] = part


def serve_last_kernel(three_ref, r3_ref, weight_ref, out_ref, fetched_ref, sems):
    rows = r3_ref.shape[0]
    fetches = fetch_blocks(weight_ref, fetched_ref, sems)
    out_ref[:, :3] = three_ref[...]
    for fetch, block in fetches:
        fetch.wait()
        out_ref[:, 3, :, block] = serve_part(fetched_ref[block, :], r3_ref[...], rows)[0]


def back_kernel(meta_ref, chosen_ref, scores_ref, hidden_ref, r0_ref, r1_ref, r2_ref, r3_ref, act_ref, score_ref, score_bf_ref):
    tokens = hidden_ref.shape[0]
    experts = scores_ref.shape[0]
    own_back = jnp.zeros(hidden_ref.shape, jnp.float32)
    for k, ref in enumerate((r0_ref, r1_ref, r2_ref, r3_ref)):
        target = column(meta_ref[k:k + 1, :].astype(jnp.float32), tokens).astype(jnp.int32)
        pick = as_pick(lax.broadcasted_iota(jnp.int32, (tokens, ref.shape[0]), 1) == target)
        own_back = own_back + jnp.dot(pick, ref[...], preferred_element_type=jnp.float32)
    onehot = lax.broadcasted_iota(jnp.int32, (experts, tokens), 0) == chosen_ref[...]
    logit = jnp.sum(jnp.where(onehot, scores_ref[...], 0.0), axis=0, keepdims=True)
    sigmoid_vals = jax.nn.sigmoid(logit)
    gate = (route_scale * sigmoid_vals).astype(jnp.bfloat16).astype(jnp.float32)
    act_ref[...] = (column(gate, tokens) * own_back).astype(jnp.bfloat16)
    route = jnp.sum(hidden_ref[...].astype(jnp.float32) * own_back, axis=1, keepdims=True)
    route_row = jnp.broadcast_to(route, (tokens, tokens)).T[:1, :]
    slope = route_row * route_scale * sigmoid_vals * (1.0 - sigmoid_vals)
    score = jnp.where(onehot, slope, 0.0)
    score_ref[...] = score
    score_bf_ref[...] = score.astype(jnp.bfloat16)


def up_kernel(early_ref, late_ref, rest_ref, score_ref, router_ref, out_ref):
    half = early_ref.shape[0] - 8
    tokens = out_ref.shape[0]
    last = tokens - rest_ref.shape[0]
    rank = column(early_ref[half:, :tokens].astype(jnp.float32)[2:3, :], tokens).astype(jnp.int32)
    pick = as_pick(lax.broadcasted_iota(jnp.int32, (tokens, tokens), 1) == rank)
    scores = score_ref[...].astype(jnp.float32).T.astype(jnp.bfloat16)
    out = jnp.dot(pick[:, :half], early_ref[:half], preferred_element_type=jnp.float32)
    out = out + jnp.dot(pick[:, half:last], late_ref[...], preferred_element_type=jnp.float32)
    out = out + jnp.dot(pick[:, last:], rest_ref[...], preferred_element_type=jnp.float32)
    out = out + jnp.dot(scores, router_ref[...], preferred_element_type=jnp.float32)
    out_ref[...] = out.astype(jnp.bfloat16)


def call(kernel, outs, *operands, scratch=()):
    space = {"held": pltpu.VMEM, "near": pltpu.HBM, "far": pltpu.HBM}
    values = [pltpu.with_memory_space_constraint(x, space[how]) for how, x in operands]
    return pl.pallas_call(
        kernel,
        out_shape=tuple(space[how](shape, dtype) for how, shape, dtype in outs),
        in_specs=[pl.BlockSpec(memory_space=pltpu.HBM if how == "far" else pltpu.VMEM) for how, _ in operands],
        out_specs=tuple(pl.BlockSpec(memory_space=pltpu.VMEM) for _ in outs),
        scratch_shapes=scratch,
        compiler_params=pltpu.CompilerParams(vmem_limit_bytes=24 * 1024 * 1024),
    )(*values)


def on_device(dims, grad_out, hidden_act, scores, expert_ids, slot_ids, counts, down_weight, router):
    ny, nz, nzl, nxc = dims
    tok = grad_out[0]
    tokens, width = tok.shape
    hidden_width = hidden_act.shape[2]
    half = tokens // 2
    rows = nxc * slots
    spare = tokens - 14 * nxc
    weight = down_weight[0]

    def lanes(pairs):
        return [(a * nxc + j, b * nxc + j) for a, b in pairs for j in range(nxc)]

    def along_z(value, distance):
        pairs = [(y * nz + z, y * nz + (z + distance) % nz) for y in range(ny) for z in range(nz)]
        return lax.ppermute(value, axes, lanes(pairs))

    def to_end(value, left):
        pairs = []
        for y in range(ny):
            for z in range(nz):
                to = y * nz + (z + nzl - left) % nz - nzl
                if to >= 0:
                    pairs.append((y * nz + z, to))
        return lax.ppermute(value, axes, lanes(pairs))

    def exchange(value):
        return lax.all_to_all(value, group, split_axis=0, concat_axis=0, tiled=True)

    def spread(value):
        return exchange(value.reshape(nxc, slots, width)).reshape(rows, width)

    def serve_three(*values):
        scratch = [pltpu.VMEM((hidden_width, width), bf16), pltpu.VMEM((3 * rows, width), bf16), pltpu.SemaphoreType.DMA((2,))]
        outs = [("held", (nxc, 3, slots, hidden_width), bf16)]
        return call(serve_three_kernel, outs, *held(*values), ("far", weight), scratch=scratch)[0]

    def serve_last(*values):
        scratch = [pltpu.VMEM((hidden_width, width), bf16), pltpu.SemaphoreType.DMA((4,))]
        outs = [("held", (nxc, 4, slots, hidden_width), bf16)]
        return call(serve_last_kernel, outs, *held(*values), ("far", weight), scratch=scratch)[0]

    def held(*values):
        return [("held", v) for v in values]

    def near_by(*values):
        return [("near", v) for v in values]

    def part(value, k):
        return value[:, k].reshape(rows, value.shape[3])

    outs = [
        ("held", (2 * rows, width), bf16),
        ("held", (half + 8, width), bf16),
        ("held", (tokens - half - spare, width), bf16),
        ("held", (spare, width), bf16),
        ("near", (8, tokens), jnp.int32),
    ]
    first, early, late, rest, meta = call(prep_kernel, outs, *near_by(expert_ids, slot_ids, counts[0], tok))
    early1 = along_z(early, -1)
    first = exchange(first.reshape(nxc, 2, slots, width))
    late1 = along_z(late, -1)
    rest = along_z(rest, nzl)
    early2 = along_z(early1, -1)
    near, up = part(first, 0), part(first, 1)
    up = along_z(up, 1)
    one = call(pack_one_kernel, [("held", (rows, width), bf16)], *held(early1, late1))[0]
    one = spread(one)
    late4 = to_end(late1, 3)
    rest = along_z(rest, nzl)
    two = call(pack_two_kernel, [("held", (rows, width), bf16)], *held(early2))[0]
    two = spread(two)
    early4 = to_end(early2, 2)
    three = serve_three(near, up, one)
    served = serve_last(three, two)
    served = exchange(served)
    rest4 = to_end(rest, nz - nzl)
    r0, r1, r3, r2 = (part(served, k) for k in range(4))
    r2 = along_z(r2, 2)
    r1 = along_z(r1, -1)
    r3 = along_z(r3, 1)
    experts = scores.shape[2]
    outs = [
        ("near", (tokens, hidden_width), bf16),
        ("near", (experts, tokens), jnp.float32),
        ("held", (experts, tokens), bf16),
    ]
    ins = near_by(meta, expert_ids, scores[0].T, hidden_act[0]) + held(r0, r1, r2, r3)
    act, score, score_bf = call(back_kernel, outs, *ins)
    late_score = to_end(score_bf, nzl)
    upstream = call(up_kernel, [("near", (tokens, width), bf16)], *held(early4, late4, rest4, late_score, router))[0]
    return act[None], score.T[None], upstream[None]


def solution(mesh):
    cut_mesh = Mesh(mesh.devices.reshape(8, 4, 4, 4, 2), axes)
    dims = (8, 16, 4, 8)
    section = ("y", "zh")
    rows = P(section, expert_axes, None)
    in_specs = (rows, rows, rows, P(section, expert_axes), P(section, expert_axes), P(section, None, None), P(expert_axes, None, None), P())

    def body(*arrays):
        return on_device(dims, *arrays)

    return jax.shard_map(body, mesh=cut_mesh, in_specs=in_specs, out_specs=(rows, rows, rows), check_vma=False)
```

```python
import jax
import jax.numpy as jnp
from jax import lax
from jax.experimental import pallas as pl
from jax.experimental.pallas import tpu as pltpu
from jax.sharding import Mesh, PartitionSpec as P


route_scale = 2.5
slots = 8
bf16 = jnp.bfloat16
axes = ("y", "zh", "zl", "x", "c")
group = ("x", "c")
expert_axes = ("zl", "x", "c")

NT = (((1,), (1,)), ((), ()))


def as_pick(mask):
    return mask.astype(jnp.float32).astype(jnp.bfloat16)


def column(row, count):
    return jnp.broadcast_to(row, (count, row.shape[1])).T[:, :1]


def prep_kernel(chosen_ref, places_ref, counts_ref, tok_ref, first_ref, early_ref, late_ref, rest_ref, meta_ref):
    tokens, width = tok_ref.shape
    half = early_ref.shape[0] - 8
    last = tokens - rest_ref.shape[0]
    experts = counts_ref.shape[0]
    rows = first_ref.shape[0]
    own = lax.axis_index(expert_axes)
    own_z = lax.axis_index("zl")
    chosen = chosen_ref[...]
    places = places_ref[...]
    onehot = lax.broadcasted_iota(jnp.int32, (experts, tokens), 0) == chosen
    own_row = lax.broadcasted_iota(jnp.int32, counts_ref.shape, 0) == own
    own_counts = jnp.where(own_row, counts_ref[...], 0).astype(jnp.float32).astype(jnp.bfloat16)
    picked = jnp.dot(own_counts, as_pick(onehot), preferred_element_type=jnp.float32)
    limit = jnp.sum(picked, axis=0, keepdims=True)
    live = places.astype(jnp.float32) < limit
    offset = (lax.shift_right_logical(chosen, 3) - own_z) & 3
    dest = chosen & 7

    def slot_of(k):
        return jnp.where(live & (offset == k), dest * slots + places, -1)

    order = lax.broadcasted_iota(jnp.int32, (1, tokens), 1)
    key = (jnp.where(live & (offset >= 2), jnp.where(offset == 2, 0, tokens), 2 * tokens) + order).astype(jnp.float32)
    key_rows = jnp.broadcast_to(key, (tokens, tokens))
    rank = jnp.sum((key_rows.T < key_rows).astype(jnp.float32), axis=0, keepdims=True)
    perm = as_pick(lax.broadcasted_iota(jnp.int32, (tokens, tokens), 0) == rank.astype(jnp.int32))
    row_id = lax.broadcasted_iota(jnp.int32, (8, tokens), 0)
    one_down = slot_of(3).astype(jnp.float32)
    two_down = slot_of(2).astype(jnp.float32)
    pair = jnp.where(row_id == 0, one_down, jnp.where(row_id == 1, two_down, 0.0)).astype(jnp.bfloat16)
    moved = lax.dot_general(pair, perm, NT, preferred_element_type=jnp.float32)

    tok = tok_ref[...]
    ordered = jnp.dot(perm, tok, preferred_element_type=jnp.float32).astype(jnp.bfloat16)
    early_ref[:half] = ordered[:half]
    early_ref[half:] = jnp.zeros((8, width), jnp.bfloat16)
    table = jnp.where(row_id < 2, moved, jnp.where(row_id == 2, rank, 0.0)).astype(jnp.bfloat16)
    early_ref[half:, :tokens] = table
    late_ref[...] = ordered[half:last]
    rest_ref[...] = ordered[last:]
    target = jnp.where(live & (offset < 2), (2 * dest + offset) * slots + places, -1)
    pick = as_pick(lax.broadcasted_iota(jnp.int32, (rows, tokens), 0) == target)
    first_ref[...] = jnp.dot(pick, tok, preferred_element_type=jnp.float32).astype(jnp.bfloat16)
    back = jnp.where(row_id == 0, slot_of(0), -1)
    for k in (1, 2, 3):
        back = jnp.where(row_id == k, slot_of(k), back)
    meta_ref[...] = back


def pack_one_kernel(early_ref, late_ref, out_ref):
    half = early_ref.shape[0] - 8
    count = half + late_ref.shape[0]
    target = early_ref[half:, :2 * half].astype(jnp.float32)[0:1, :].astype(jnp.int32)
    pick = as_pick(lax.broadcasted_iota(jnp.int32, (out_ref.shape[0], 2 * half), 0) == target)
    out = jnp.dot(pick[:, :half], early_ref[:half], preferred_element_type=jnp.float32)
    out = out + jnp.dot(pick[:, half:count], late_ref[...], preferred_element_type=jnp.float32)
    out_ref[...] = out.astype(jnp.bfloat16)


def pack_two_kernel(early_ref, out_ref):
    half = early_ref.shape[0] - 8
    target = early_ref[half:, :2 * half].astype(jnp.float32)[1:2, :].astype(jnp.int32)
    pick = as_pick(lax.broadcasted_iota(jnp.int32, (out_ref.shape[0], 2 * half), 0) == target)
    out_ref[...] = jnp.dot(pick[:, :half], early_ref[:half], preferred_element_type=jnp.float32).astype(jnp.bfloat16)


def serve_part(weight, held, rows):
    found = lax.dot_general(weight, held, NT, preferred_element_type=jnp.float32).T
    parts = []
    for k in range(found.shape[0] // rows):
        part = found[k * rows:(k + 1) * rows].reshape(rows // slots, slots, weight.shape[0])
        parts.append(part.astype(jnp.bfloat16))
    return parts


def serve_kernel(r0_ref, r1_ref, r2_ref, r3_ref, weight_ref, out_ref, fetched_ref, held_ref, sems):
    rows = r0_ref.shape[0]
    count = sems.shape[0]
    step = weight_ref.shape[0] // count
    blocks = [pl.ds(j * step, step) for j in range(count)]
    fetches = [pltpu.make_async_copy(weight_ref.at[blocks[j]], fetched_ref.at[blocks[j]], sems.at[j]) for j in range(count)]
    fetches[0].start()
    fetches[1].start()
    for k, ref in enumerate((r0_ref, r1_ref, r2_ref, r3_ref)):
        held_ref[k * rows:(k + 1) * rows] = ref[...]
    for j in range(count):
        fetches[j].wait()
        if j + 2 < count:
            fetches[j + 2].start()
        for k, part in enumerate(serve_part(fetched_ref[blocks[j], :], held_ref[...], rows)):
            out_ref[:, k, :, blocks[j]] = part


def back_kernel(meta_ref, chosen_ref, scores_ref, hidden_ref, r0_ref, r1_ref, r2_ref, r3_ref, act_ref, score_ref, score_bf_ref):
    tokens = hidden_ref.shape[0]
    experts = scores_ref.shape[0]
    own_back = jnp.zeros(hidden_ref.shape, jnp.float32)
    for k, ref in enumerate((r0_ref, r1_ref, r2_ref, r3_ref)):
        target = column(meta_ref[k:k + 1, :].astype(jnp.float32), tokens).astype(jnp.int32)
        pick = as_pick(lax.broadcasted_iota(jnp.int32, (tokens, ref.shape[0]), 1) == target)
        own_back = own_back + jnp.dot(pick, ref[...], preferred_element_type=jnp.float32)
    onehot = lax.broadcasted_iota(jnp.int32, (experts, tokens), 0) == chosen_ref[...]
    logit = jnp.sum(jnp.where(onehot, scores_ref[...], 0.0), axis=0, keepdims=True)
    sigmoid_vals = jax.nn.sigmoid(logit)
    gate = (route_scale * sigmoid_vals).astype(jnp.bfloat16).astype(jnp.float32)
    act_ref[...] = (column(gate, tokens) * own_back).astype(jnp.bfloat16)
    route = jnp.sum(hidden_ref[...].astype(jnp.float32) * own_back, axis=1, keepdims=True)
    route_row = jnp.broadcast_to(route, (tokens, tokens)).T[:1, :]
    slope = route_row * route_scale * sigmoid_vals * (1.0 - sigmoid_vals)
    score = jnp.where(onehot, slope, 0.0)
    score_ref[...] = score
    score_bf_ref[...] = score.astype(jnp.bfloat16)


def up_kernel(early_ref, late_ref, rest_ref, score_ref, router_ref, out_ref):
    half = early_ref.shape[0] - 8
    tokens = out_ref.shape[0]
    last = tokens - rest_ref.shape[0]
    rank = column(early_ref[half:, :tokens].astype(jnp.float32)[2:3, :], tokens).astype(jnp.int32)
    pick = as_pick(lax.broadcasted_iota(jnp.int32, (tokens, tokens), 1) == rank)
    scores = score_ref[...].astype(jnp.float32).T.astype(jnp.bfloat16)
    out = jnp.dot(pick[:, :half], early_ref[:half], preferred_element_type=jnp.float32)
    out = out + jnp.dot(pick[:, half:last], late_ref[...], preferred_element_type=jnp.float32)
    out = out + jnp.dot(pick[:, last:], rest_ref[...], preferred_element_type=jnp.float32)
    out = out + jnp.dot(scores, router_ref[...], preferred_element_type=jnp.float32)
    out_ref[...] = out.astype(jnp.bfloat16)


def call(kernel, outs, *operands, scratch=()):
    space = {"held": pltpu.VMEM, "near": pltpu.HBM, "far": pltpu.HBM}
    values = [pltpu.with_memory_space_constraint(x, space[how]) for how, x in operands]
    return pl.pallas_call(
        kernel,
        out_shape=tuple(space[how](shape, dtype) for how, shape, dtype in outs),
        in_specs=[pl.BlockSpec(memory_space=pltpu.HBM if how == "far" else pltpu.VMEM) for how, _ in operands],
        out_specs=tuple(pl.BlockSpec(memory_space=pltpu.VMEM) for _ in outs),
        scratch_shapes=scratch,
        compiler_params=pltpu.CompilerParams(vmem_limit_bytes=24 * 1024 * 1024),
    )(*values)


def on_device(dims, grad_out, hidden_act, scores, expert_ids, slot_ids, counts, down_weight, router):
    ny, nz, nzl, nxc = dims
    tok = grad_out[0]
    tokens, width = tok.shape
    hidden_width = hidden_act.shape[2]
    half = tokens // 2
    rows = nxc * slots
    spare = tokens - 14 * nxc
    weight = down_weight[0]

    def lanes(pairs):
        return [(a * nxc + j, b * nxc + j) for a, b in pairs for j in range(nxc)]

    def along_z(value, distance):
        pairs = [(y * nz + z, y * nz + (z + distance) % nz) for y in range(ny) for z in range(nz)]
        return lax.ppermute(value, axes, lanes(pairs))

    def to_end(value, left):
        pairs = []
        for y in range(ny):
            for z in range(nz):
                to = y * nz + (z + nzl - left) % nz - nzl
                if to >= 0:
                    pairs.append((y * nz + z, to))
        return lax.ppermute(value, axes, lanes(pairs))

    def exchange(value):
        return lax.all_to_all(value, group, split_axis=0, concat_axis=0, tiled=True)

    def spread(value):
        return exchange(value.reshape(nxc, slots, width)).reshape(rows, width)

    def serve(*values):
        scratch = [pltpu.VMEM((hidden_width, width), bf16), pltpu.VMEM((4 * rows, width), bf16), pltpu.SemaphoreType.DMA((4,))]
        outs = [("held", (nxc, 4, slots, hidden_width), bf16)]
        return call(serve_kernel, outs, *held(*values), ("far", weight), scratch=scratch)[0]

    def held(*values):
        return [("held", v) for v in values]

    def near_by(*values):
        return [("near", v) for v in values]

    def part(value, k):
        return value[:, k].reshape(rows, value.shape[3])

    outs = [
        ("held", (2 * rows, width), bf16),
        ("held", (half + 8, width), bf16),
        ("held", (tokens - half - spare, width), bf16),
        ("held", (spare, width), bf16),
        ("near", (8, tokens), jnp.int32),
    ]
    first, early, late, rest, meta = call(prep_kernel, outs, *near_by(expert_ids, slot_ids, counts[0], tok))
    early1 = along_z(early, -1)
    first = exchange(first.reshape(nxc, 2, slots, width))
    late1 = along_z(late, -1)
    rest = along_z(rest, (nz - nzl) // 2)
    early2 = along_z(early1, -1)
    near, up = part(first, 0), part(first, 1)
    up = along_z(up, 1)
    one = call(pack_one_kernel, [("held", (rows, width), bf16)], *held(early1, late1))[0]
    one = spread(one)
    late4 = to_end(late1, 3)
    rest4 = to_end(rest, nzl + (nz - nzl) // 2)
    two = call(pack_two_kernel, [("held", (rows, width), bf16)], *held(early2))[0]
    two = spread(two)
    early4 = to_end(early2, 2)
    served = serve(near, up, one, two)
    served = exchange(served)
    r0, r1, r3, r2 = (part(served, k) for k in range(4))
    r2 = along_z(r2, 2)
    r1 = along_z(r1, -1)
    r3 = along_z(r3, 1)
    experts = scores.shape[2]
    outs = [
        ("near", (tokens, hidden_width), bf16),
        ("near", (experts, tokens), jnp.float32),
        ("held", (experts, tokens), bf16),
    ]
    ins = near_by(meta, expert_ids, scores[0].T, hidden_act[0]) + held(r0, r1, r2, r3)
    act, score, score_bf = call(back_kernel, outs, *ins)
    late_score = to_end(score_bf, nzl)
    upstream = call(up_kernel, [("near", (tokens, width), bf16)], *held(early4, late4, rest4, late_score, router))[0]
    return act[None], score.T[None], upstream[None]


def solution(mesh):
    cut_mesh = Mesh(mesh.devices.reshape(8, 4, 4, 4, 2), axes)
    dims = (8, 16, 4, 8)
    section = ("y", "zh")
    rows = P(section, expert_axes, None)
    in_specs = (rows, rows, rows, P(section, expert_axes), P(section, expert_axes), P(section, None, None), P(expert_axes, None, None), P())

    def body(*arrays):
        return on_device(dims, *arrays)

    return jax.shard_map(body, mesh=cut_mesh, in_specs=in_specs, out_specs=(rows, rows, rows), check_vma=False)
```

```python
import jax
import jax.numpy as jnp
from jax import lax
from jax.experimental import pallas as pl
from jax.experimental.pallas import tpu as pltpu
from jax.sharding import Mesh, PartitionSpec as P


route_scale = 2.5
slots = 8
bf16 = jnp.bfloat16
axes = ("y", "zh", "zl", "x", "c")
group = ("x", "c")
expert_axes = ("zl", "x", "c")

NT = (((1,), (1,)), ((), ()))


def as_pick(mask):
    return mask.astype(jnp.float32).astype(jnp.bfloat16)


def column(row, count):
    return jnp.broadcast_to(row, (count, row.shape[1])).T[:, :1]


def prep_kernel(chosen_ref, places_ref, counts_ref, tok_ref, first_ref, early_ref, late_ref, meta_ref):
    tokens, width = tok_ref.shape
    half = late_ref.shape[0]
    experts = counts_ref.shape[0]
    rows = first_ref.shape[0]
    own = lax.axis_index(expert_axes)
    own_z = lax.axis_index("zl")
    chosen = chosen_ref[...]
    places = places_ref[...]
    onehot = lax.broadcasted_iota(jnp.int32, (experts, tokens), 0) == chosen
    own_row = lax.broadcasted_iota(jnp.int32, counts_ref.shape, 0) == own
    own_counts = jnp.where(own_row, counts_ref[...], 0).astype(jnp.float32).astype(jnp.bfloat16)
    picked = jnp.dot(own_counts, as_pick(onehot), preferred_element_type=jnp.float32)
    limit = jnp.sum(picked, axis=0, keepdims=True)
    live = places.astype(jnp.float32) < limit
    offset = (lax.shift_right_logical(chosen, 3) - own_z) & 3
    dest = chosen & 7

    def slot_of(k):
        return jnp.where(live & (offset == k), dest * slots + places, -1)

    order = lax.broadcasted_iota(jnp.int32, (1, tokens), 1)
    key = (jnp.where(live & (offset == 2), 0, tokens) + order).astype(jnp.float32)
    key_rows = jnp.broadcast_to(key, (tokens, tokens))
    rank = jnp.sum((key_rows.T < key_rows).astype(jnp.float32), axis=0, keepdims=True)
    perm = as_pick(lax.broadcasted_iota(jnp.int32, (tokens, tokens), 0) == rank.astype(jnp.int32))
    row_id = lax.broadcasted_iota(jnp.int32, (8, tokens), 0)
    one_down = slot_of(3).astype(jnp.float32)
    two_down = slot_of(2).astype(jnp.float32)
    pair = jnp.where(row_id == 0, one_down, jnp.where(row_id == 1, two_down, 0.0)).astype(jnp.bfloat16)
    moved = lax.dot_general(pair, perm, NT, preferred_element_type=jnp.float32)

    tok = tok_ref[...]
    ordered = jnp.dot(perm, tok, preferred_element_type=jnp.float32).astype(jnp.bfloat16)
    early_ref[:half] = ordered[:half]
    early_ref[half:] = jnp.zeros((8, width), jnp.bfloat16)
    early_ref[half:, :tokens] = moved.astype(jnp.bfloat16)
    late_ref[...] = ordered[half:]
    target = jnp.where(live & (offset < 2), (2 * dest + offset) * slots + places, -1)
    pick = as_pick(lax.broadcasted_iota(jnp.int32, (rows, tokens), 0) == target)
    first_ref[...] = jnp.dot(pick, tok, preferred_element_type=jnp.float32).astype(jnp.bfloat16)
    back = jnp.where(row_id == 0, slot_of(0), -1)
    for k in (1, 2, 3):
        back = jnp.where(row_id == k, slot_of(k), back)
    meta_ref[...] = jnp.where(row_id == 4, rank.astype(jnp.int32), back)


def pack_one_kernel(early_ref, late_ref, out_ref):
    half = late_ref.shape[0]
    tokens = 2 * half
    target = early_ref[half:, :tokens].astype(jnp.float32)[0:1, :].astype(jnp.int32)
    pick = as_pick(lax.broadcasted_iota(jnp.int32, (out_ref.shape[0], tokens), 0) == target)
    out = jnp.dot(pick[:, :half], early_ref[:half], preferred_element_type=jnp.float32)
    out = out + jnp.dot(pick[:, half:], late_ref[...], preferred_element_type=jnp.float32)
    out_ref[...] = out.astype(jnp.bfloat16)


def pack_two_kernel(early_ref, out_ref):
    half = early_ref.shape[0] - 8
    target = early_ref[half:, :2 * half].astype(jnp.float32)[1:2, :].astype(jnp.int32)
    pick = as_pick(lax.broadcasted_iota(jnp.int32, (out_ref.shape[0], 2 * half), 0) == target)
    out_ref[...] = jnp.dot(pick[:, :half], early_ref[:half], preferred_element_type=jnp.float32).astype(jnp.bfloat16)


def serve_kernel(r0_ref, r1_ref, r2_ref, r3_ref, weight_ref, out_ref, held_ref, fetched_ref, sems):
    rows = r0_ref.shape[0]
    count = sems.shape[0]
    step = weight_ref.shape[0] // count
    blocks = [pl.ds(j * step, step) for j in range(count)]
    fetches = [pltpu.make_async_copy(weight_ref.at[blocks[j]], fetched_ref.at[blocks[j]], sems.at[j]) for j in range(count)]
    fetches[0].start()
    fetches[1].start()
    for k, ref in enumerate((r0_ref, r1_ref, r2_ref, r3_ref)):
        held_ref[k * rows:(k + 1) * rows] = ref[...]
    for j in range(count):
        fetches[j].wait()
        if j + 2 < count:
            fetches[j + 2].start()
        found = lax.dot_general(fetched_ref[blocks[j], :], held_ref[...], NT, preferred_element_type=jnp.float32).T
        for k in range(4):
            part = found[k * rows:(k + 1) * rows].reshape(rows // slots, slots, step)
            out_ref[:, k, :, blocks[j]] = part.astype(jnp.bfloat16)


def back_kernel(meta_ref, chosen_ref, scores_ref, hidden_ref, r0_ref, r1_ref, r2_ref, r3_ref, act_ref, score_ref, score_bf_ref):
    tokens = hidden_ref.shape[0]
    experts = scores_ref.shape[0]
    own_back = jnp.zeros(hidden_ref.shape, jnp.float32)
    for k, ref in enumerate((r0_ref, r1_ref, r2_ref, r3_ref)):
        target = column(meta_ref[k:k + 1, :].astype(jnp.float32), tokens).astype(jnp.int32)
        pick = as_pick(lax.broadcasted_iota(jnp.int32, (tokens, ref.shape[0]), 1) == target)
        own_back = own_back + jnp.dot(pick, ref[...], preferred_element_type=jnp.float32)
    onehot = lax.broadcasted_iota(jnp.int32, (experts, tokens), 0) == chosen_ref[...]
    logit = jnp.sum(jnp.where(onehot, scores_ref[...], 0.0), axis=0, keepdims=True)
    sigmoid_vals = jax.nn.sigmoid(logit)
    gate = (route_scale * sigmoid_vals).astype(jnp.bfloat16).astype(jnp.float32)
    act_ref[...] = (column(gate, tokens) * own_back).astype(jnp.bfloat16)
    route = jnp.sum(hidden_ref[...].astype(jnp.float32) * own_back, axis=1, keepdims=True)
    route_row = jnp.broadcast_to(route, (tokens, tokens)).T[:1, :]
    slope = route_row * route_scale * sigmoid_vals * (1.0 - sigmoid_vals)
    score = jnp.where(onehot, slope, 0.0)
    score_ref[...] = score
    score_bf_ref[:experts] = score.astype(jnp.bfloat16)
    order = jnp.broadcast_to(meta_ref[4:5, :].astype(jnp.float32), (8, tokens))
    score_bf_ref[experts:] = order.astype(jnp.bfloat16)


def up_kernel(early_ref, late_ref, score_ref, router_ref, out_ref):
    half = early_ref.shape[0]
    tokens = out_ref.shape[0]
    experts = router_ref.shape[0]
    rank = column(score_ref[experts:, :].astype(jnp.float32)[:1, :], tokens).astype(jnp.int32)
    pick = as_pick(lax.broadcasted_iota(jnp.int32, (tokens, tokens), 1) == rank)
    scores = score_ref[:experts, :].astype(jnp.float32).T.astype(jnp.bfloat16)
    out = jnp.dot(pick[:, :half], early_ref[...], preferred_element_type=jnp.float32)
    out = out + jnp.dot(pick[:, half:], late_ref[...], preferred_element_type=jnp.float32)
    out = out + jnp.dot(scores, router_ref[...], preferred_element_type=jnp.float32)
    out_ref[...] = out.astype(jnp.bfloat16)


def call(kernel, outs, *operands, scratch=()):
    space = {"held": pltpu.VMEM, "near": pltpu.HBM, "far": pltpu.HBM}
    values = [pltpu.with_memory_space_constraint(x, space[how]) for how, x in operands]
    return pl.pallas_call(
        kernel,
        out_shape=tuple(space[how](shape, dtype) for how, shape, dtype in outs),
        in_specs=[pl.BlockSpec(memory_space=pltpu.HBM if how == "far" else pltpu.VMEM) for how, _ in operands],
        out_specs=tuple(pl.BlockSpec(memory_space=pltpu.VMEM) for _ in outs),
        scratch_shapes=scratch,
        compiler_params=pltpu.CompilerParams(vmem_limit_bytes=24 * 1024 * 1024),
    )(*values)


def on_device(dims, grad_out, hidden_act, scores, expert_ids, slot_ids, counts, down_weight, router):
    ny, nz, nzl, nxc = dims
    tok = grad_out[0]
    tokens, width = tok.shape
    hidden_width = hidden_act.shape[2]
    half = tokens // 2
    rows = nxc * slots
    weight = down_weight[0]

    def lanes(pairs):
        return [(a * nxc + j, b * nxc + j) for a, b in pairs for j in range(nxc)]

    def along_z(value, distance):
        pairs = [(y * nz + z, y * nz + (z + distance) % nz) for y in range(ny) for z in range(nz)]
        return lax.ppermute(value, axes, lanes(pairs))

    def to_end(value, left):
        pairs = []
        for y in range(ny):
            for z in range(nz):
                to = y * nz + (z + nzl - left) % nz - nzl
                if to >= 0:
                    pairs.append((y * nz + z, to))
        return lax.ppermute(value, axes, lanes(pairs))

    def exchange(value):
        return lax.all_to_all(value, group, split_axis=0, concat_axis=0, tiled=True)

    def spread(value):
        return exchange(value.reshape(nxc, slots, width)).reshape(rows, width)

    def serve(*values):
        scratch = [
            pltpu.VMEM((4 * rows, width), bf16),
            pltpu.VMEM((hidden_width, width), bf16),
            pltpu.SemaphoreType.DMA((4,)),
        ]
        outs = [("held", (nxc, 4, slots, hidden_width), bf16)]
        return call(serve_kernel, outs, *held(*values), ("far", weight), scratch=scratch)[0]

    def held(*values):
        return [("held", v) for v in values]

    def near_by(*values):
        return [("near", v) for v in values]

    def part(value, k):
        return value[:, k].reshape(rows, value.shape[3])

    outs = [
        ("held", (2 * rows, width), bf16),
        ("held", (half + 8, width), bf16),
        ("held", (half, width), bf16),
        ("near", (8, tokens), jnp.int32),
    ]
    first, early, late, meta = call(prep_kernel, outs, *near_by(expert_ids, slot_ids, counts[0], tok))
    early1 = along_z(early, -1)
    first = exchange(first.reshape(nxc, 2, slots, width))
    late1 = along_z(late, -1)
    early2 = along_z(early1, -1)
    near, up = part(first, 0), part(first, 1)
    up = along_z(up, 1)
    one = call(pack_one_kernel, [("held", (rows, width), bf16)], *held(early1, late1))[0]
    one = spread(one)
    late4 = to_end(late1, 3)
    two = call(pack_two_kernel, [("held", (rows, width), bf16)], *held(early2))[0]
    two = spread(two)
    early4 = to_end(early2[:half], 2)
    served = serve(near, up, one, two)
    served = exchange(served)
    r0, r1, r3, r2 = (part(served, k) for k in range(4))
    r2 = along_z(r2, 2)
    r1 = along_z(r1, -1)
    r3 = along_z(r3, 1)
    experts = scores.shape[2]
    outs = [
        ("near", (tokens, hidden_width), bf16),
        ("near", (experts, tokens), jnp.float32),
        ("held", (experts + 8, tokens), bf16),
    ]
    ins = near_by(meta, expert_ids, scores[0].T, hidden_act[0]) + held(r0, r1, r2, r3)
    act, score, score_bf = call(back_kernel, outs, *ins)
    late_score = to_end(score_bf, nzl)
    upstream = call(up_kernel, [("near", (tokens, width), bf16)], *held(early4, late4, late_score, router))[0]
    return act[None], score.T[None], upstream[None]


def solution(mesh):
    cut_mesh = Mesh(mesh.devices.reshape(8, 4, 4, 4, 2), axes)
    dims = (8, 16, 4, 8)
    section = ("y", "zh")
    rows = P(section, expert_axes, None)
    in_specs = (rows, rows, rows, P(section, expert_axes), P(section, expert_axes), P(section, None, None), P(expert_axes, None, None), P())

    def body(*arrays):
        return on_device(dims, *arrays)

    return jax.shard_map(body, mesh=cut_mesh, in_specs=in_specs, out_specs=(rows, rows, rows), check_vma=False)
```
